32 devices in a mesh: prow: 4 (over y, core), pcol: 8 (over z, x).
Axes of the slice: x: 2, y: 2, z: 4, core: 2. Of those that a mesh axis runs over, the one named last changes fastest.
Arguments:
- inverse_cov: bfloat16 [8192, 8192], P('prow', 'pcol'), may hold values from -0.5 to 4.5, as said below
- cosines: float32 [8192, 8192], P('prow', 'pcol'), may hold values from -1 to 1, as said below
- sky_maps: bfloat16 [8192, 192], P('pcol'), may hold values from -6 to 6
Outputs:
- filtered: bfloat16 [8192, 192], P('prow')
- spectra: float32 [64, 192], replicated
The draws below stay inside these ranges and needn't reach their ends.
Inputs may be any that keep to these rules, and one draw needn't show every extreme that they name: `inverse_cov`: symmetric, with a dominant diagonal. `cosines`: symmetric.
All inputs are finite; a program needn't handle non-finite values.
Results may differ from the reference program's by a relative error of at most 0.0033.
Values may be sent and summed in bfloat16 or wider, within the bound.
A program may use at most 128 MiB of HBM per device.

```python
import math
import jax
import jax.numpy as jnp
from jax import lax

NPIX = 8192
MAPS = 192
L = 64
LMIN = 2


def draw_inverse_cov(key, part):
    first_key, second_key = jax.random.split(jax.random.fold_in(key, 11))
    noise = jax.random.truncated_normal(first_key, -6.0, 6.0, (NPIX, NPIX), jnp.float32) * (0.5 / math.sqrt(NPIX))
    symmetric = noise + noise.T
    diagonal = jax.random.uniform(second_key, (NPIX,), jnp.float32, 1.0, 2.0)
    return (symmetric + jnp.diag(diagonal)).astype(jnp.bfloat16)


def draw_cosines(key, part):
    vector_key, rough_key = jax.random.split(jax.random.fold_in(key, 23))
    vectors = jax.random.normal(vector_key, (NPIX, 3), jnp.float32)
    rough = jax.random.truncated_normal(rough_key, -4.0, 4.0, (NPIX, NPIX), jnp.float32) * 0.05
    units = vectors / jnp.sqrt(jnp.sum(vectors * vectors, axis=1, keepdims=True) + 1e-12)
    product = jnp.dot(units, units.T, precision=lax.Precision.HIGHEST)
    return jnp.clip(product + rough + rough.T, -1.0, 1.0)


def shard_levels(rng, extent, pieces, smallest, high):
    level = 1.0
    for dim, shards_of in pieces:
        steps = jax.random.uniform(jax.random.fold_in(jax.random.fold_in(rng, 6), dim), (shards_of,), jnp.float32, smallest / len(pieces), high / len(pieces))
        level = level * jnp.repeat(jnp.exp(steps), extent[dim] // shards_of).reshape((-1,) + (1,) * (len(extent) - 1 - dim))
    return level


def normal_values(rng, shape, scale, limit, cuts=(), kind=jnp.bfloat16):
    values = scale * jax.random.normal(rng, shape, jnp.float32)
    if cuts:
        values = values * shard_levels(rng, shape, cuts, -0.22, 0.18)
    return jnp.clip(values, -limit, limit).astype(kind)


def setup_inputs(seed: int = 0) -> dict:
    streams_of = jax.random.split(jax.random.key(seed), 4)
    inverse_cov = draw_inverse_cov(jax.random.fold_in(streams_of[3], 71), 0)
    cosines = draw_cosines(jax.random.fold_in(streams_of[3], 71), 0)
    sky_maps = normal_values(streams_of[2], (NPIX, MAPS), 1.0, 6.0, ((0, 8),))
    return {"inverse_cov": inverse_cov, "cosines": cosines, "sky_maps": sky_maps}


def next_legendre(previous, current, cosine, degree):
    return ((2.0 * degree - 1.0) * cosine * current - (degree - 1.0) * previous) / degree


def reference(inverse_cov, cosines, sky_maps):
    filtered = jnp.dot(inverse_cov, sky_maps, preferred_element_type=jnp.float32).astype(jnp.bfloat16)
    maps_f32 = filtered.astype(jnp.float32)
    blocks = 8
    size_rows = NPIX // blocks
    degrees = (jnp.arange(L) + LMIN).astype(jnp.float32)

    def block_spectra(block_index):
        first_row = (block_index * size_rows).astype(jnp.int32)
        cosine = lax.dynamic_slice_in_dim(cosines, first_row, size_rows, 0)
        rows_f32 = lax.dynamic_slice_in_dim(maps_f32, first_row, size_rows, 0)
        previous = jnp.ones_like(cosine)
        current = cosine
        for low_degree in range(2, LMIN):
            next_term = next_legendre(previous, current, cosine, jnp.float32(low_degree))
            previous, current = current, next_term

        def advance(carried, degree):
            previous, current = carried
            next_term = next_legendre(previous, current, cosine, degree)
            product = jnp.dot(next_term.astype(jnp.bfloat16), filtered, preferred_element_type=jnp.float32)
            spectrum = jnp.sum(rows_f32 * product, axis=0) * ((2.0 * degree + 1.0) / NPIX)
            return (current, next_term), spectrum

        carried, values = lax.scan(advance, (previous, current), degrees)
        return values

    per_block = lax.map(block_spectra, jnp.arange(blocks, dtype=jnp.int32))
    return filtered, jnp.sum(per_block, axis=0)
```

```python
import functools
import math
import random

import jax
import jax.numpy as jnp
import numpy as np
from jax import lax
from jax.experimental import pallas as pl
from jax.experimental.pallas import tpu as pltpu
from jax.sharding import PartitionSpec as P

L = 64
LMIN = 2
TILE = 256
STRIP = 16
LOW = 11
HIGH = 6
LEVELS = LOW * HIGH


def transform_matrix(npix, devices):
    top = LMIN + L - 1
    each = -(-L // devices)
    a = [math.comb(2 * k, k) / 4.0**k for k in range(top + 1)]
    product = np.zeros((LEVELS, LEVELS))
    for k in range(LEVELS):
        high, low = divmod(k, LOW)
        product[k, low * HIGH + high] = 1
        if high and low:
            product[k, low * HIGH + high] = 2
            product[k] -= product[high * LOW - low]
    out = np.zeros((devices * each, LEVELS))
    for l in range(LMIN, top + 1):
        owner, place = divmod(l - LMIN, each)
        row = out[owner * each + place]
        for k in range(l + 1):
            row[abs(l - 2 * k)] += a[k] * a[l - k]
        row *= (2 * l + 1) / npix
    return (out @ product).astype(np.float32), each


def pair_up(tiles, n):
    items = []
    for col in range(n):
        mine = sorted((t for t in tiles if t[1] == col), key=lambda t: t[0])
        for k in range(0, len(mine), 2):
            first = mine[k]
            second = mine[k + 1] if k + 1 < len(mine) else (first[0], col, 0)
            items.append((first[0], second[0], first[2], second[2], col))
    return items


def work_tables(n):
    lower = [[(h * n + i, j, 2) for i in range(n) for j in range(n)] for h in range(2)]
    rng = random.Random(0)
    best = None
    for _ in range(20000):
        sets = []
        cross = [[rng.random() < 0.5 for _ in range(n)] for _ in range(n)]
        for h in range(2):
            tiles = []
            for i in range(n):
                tiles.append((h * n + i, i, 1))
                for j in range(i):
                    a, b = (i, j) if rng.random() < 0.5 else (j, i)
                    tiles.append((h * n + a, b, 2))
                for j in range(n):
                    if h == 0 and cross[i][j]:
                        tiles.append((n + i, j, 2))
                    if h == 1 and not cross[i][j]:
                        tiles.append((j, i, 2))
            sets.append(pair_up(tiles, n))
        cost = max(len(s) for s in sets)
        if best is None or cost < best[0]:
            best = (cost, sets)
        if 2 * cost <= n * n + n // 2 + 1:
            break
    kinds = [pair_up(lower[0], n), pair_up(lower[1], n), pair_up(lower[1], n), pair_up(lower[0], n)] + best[1]
    longest = max(len(k) for k in kinds)
    table = np.zeros((len(kinds), longest + 1, 5), np.int32)
    for k, items in enumerate(kinds):
        table[k, : len(items)] = items
    counts = np.array([len(k) for k in kinds], np.int32)
    return table.reshape(-1), counts, longest + 1


def moments_kernel(
    stride, longest, table, counts, cos_hbm, ft, fct, out,
    xbuf, buf_a, buf_b, lhs, fj, acc, sem,
):
    r = lax.axis_index("prow")
    c = lax.axis_index("pcol")
    q, h = c // 2, c % 2
    kind = jnp.where(r > q, h, jnp.where(r < q, 2 + h, 4 + h))
    n_items = counts[kind]
    n_strips = 2 * TILE // STRIP

    def field(item, f):
        return table[(kind * stride + item) * 5 + f]

    def tile_copy(item, half):
        row = pl.multiple_of(field(item, half) * TILE, TILE)
        col = pl.multiple_of(field(item, 4) * TILE, TILE)
        return pltpu.make_async_copy(
            cos_hbm.at[pl.ds(row, TILE), pl.ds(col, TILE)],
            xbuf.at[item, pl.ds(half * TILE, TILE)],
            sem.at[item, half],
        )

    def fetch(item, carry):
        tile_copy(item, 0).start()
        tile_copy(item, 1).start()
        return carry

    def landed(item):
        @pl.when(item < n_items)
        def _():
            tile_copy(item, 0).wait()
            tile_copy(item, 1).wait()

    def set_operands(item):
        col = pl.multiple_of(field(item, 4) * TILE, TILE)
        for half in range(2):
            row = pl.multiple_of(field(item, half) * TILE, TILE)
            weight = field(item, 2 + half).astype(jnp.float32)
            value = ft[:, pl.ds(row, TILE)].astype(jnp.float32) * weight
            lhs[:, half * TILE : (half + 1) * TILE] = value.astype(jnp.bfloat16)
        fj[...] = fct[:, pl.ds(col, TILE)].astype(jnp.float32)

    def gen_strip(buf, item, s):
        rows = pl.ds(pl.multiple_of(s * STRIP, STRIP), STRIP)
        x = xbuf[item, rows, :]
        xx = x + x
        buf[1, rows, :] = x.astype(jnp.bfloat16)
        p, t = x, xx * x - 1.0
        for k in range(2, LOW):
            buf[k, rows, :] = t.astype(jnp.bfloat16)
            p, t = t, xx * t - p
        yy = t + t
        buf[LOW, rows, :] = t.astype(jnp.bfloat16)
        p, t = t, yy * t - 1.0
        for k in range(2, HIGH):
            buf[LOW + k - 1, rows, :] = t.astype(jnp.bfloat16)
            p, t = t, yy * t - p

    def item_pass(item, use, gen):
        following = jnp.minimum(item + 1, n_items - 1)
        landed(item + 1)
        set_operands(item)

        half_tile = TILE // 2
        done = 0
        for level in range(LEVELS):
            k, g = divmod(level, HIGH)
            upto = (level + 1) * n_strips // LEVELS
            for s in range(done, upto):
                gen_strip(gen, following, s)
            done = upto
            if k == 0:
                rhs = use[LOW + g - 1] if g else use[0]
            else:
                rhs = use[LOW + g - 1] * use[k] if g else use[k]
            image = jnp.dot(lhs[...], rhs, preferred_element_type=jnp.float32)
            prod = image * fj[...]
            folded = prod[:, :half_tile] + prod[:, half_tile:]
            acc[level] += folded
            xbuf[longest, 0:8, 0:half_tile] = folded[0:8, :]

    lax.fori_loop(0, n_items, fetch, 0)
    acc[...] = jnp.zeros_like(acc)
    for buf in (buf_a, buf_b):
        buf[0] = jnp.ones(buf.shape[1:], buf.dtype)
    landed(0)

    def first(s, carry):
        gen_strip(buf_a, 0, s)
        return carry

    lax.fori_loop(0, n_strips, first, 0, unroll=4)

    def two_items(pair, carry):
        item_pass(2 * pair, buf_a, buf_b)

        @pl.when(2 * pair + 1 < n_items)
        def _():
            item_pass(2 * pair + 1, buf_b, buf_a)

        return carry

    lax.fori_loop(0, (n_items + 1) // 2, two_items, 0)
    out[...] = jnp.sum(acc[...], axis=-1)


def spectra_moments(cosines, ft, fct):
    maps = ft.shape[0]
    n = cosines.shape[1] // TILE
    table, counts, stride = work_tables(n)
    longest = int(counts.max())
    vmem = pl.BlockSpec(memory_space=pltpu.VMEM)
    smem = pl.BlockSpec(memory_space=pltpu.SMEM)
    return pl.pallas_call(
        functools.partial(moments_kernel, stride, longest),
        out_shape=jax.ShapeDtypeStruct((LEVELS, maps), jnp.float32),
        in_specs=[smem, smem, pl.BlockSpec(memory_space=pl.ANY), vmem, vmem],
        out_specs=vmem,
        scratch_shapes=[
            pltpu.VMEM((longest + 1, 2 * TILE, TILE), jnp.float32),
            pltpu.VMEM((LOW + HIGH - 1, 2 * TILE, TILE), jnp.bfloat16),
            pltpu.VMEM((LOW + HIGH - 1, 2 * TILE, TILE), jnp.bfloat16),
            pltpu.VMEM((maps, 2 * TILE), jnp.bfloat16),
            pltpu.VMEM((maps, TILE), jnp.float32),
            pltpu.VMEM((LEVELS, maps, TILE // 2), jnp.float32),
            pltpu.SemaphoreType.DMA((longest, 2)),
        ],
        compiler_params=pltpu.CompilerParams(vmem_limit_bytes=48 * 2**20),
        name="moments",
    )(jnp.asarray(table), jnp.asarray(counts), cosines, ft, fct)


MESH = pl.DeviceIdType.MESH


def spread_kernel(n_q, block, out, far_send, near_send, far_recv, side_send, side_recv):
    r = lax.axis_index("prow")
    c = lax.axis_index("pcol")
    q, h = c // 2, c % 2
    width = block.shape[1]
    pieces = far_recv.shape[0]
    step = width // pieces
    partner = (r, c + 1 - 2 * h)
    above, below = (r, c + 2), (r, c - 2)
    has_above, has_below = q < n_q - 1, q > 0
    barrier = pltpu.get_barrier_semaphore()
    pl.semaphore_signal(barrier, inc=1, device_id=partner, device_id_type=MESH)

    @pl.when(has_above)
    def _():
        pl.semaphore_signal(barrier, inc=1, device_id=above, device_id_type=MESH)

    @pl.when(has_below)
    def _():
        pl.semaphore_signal(barrier, inc=1, device_id=below, device_id_type=MESH)

    pl.semaphore_wait(barrier, 1 + has_above.astype(jnp.int32) + has_below.astype(jnp.int32))

    source = q == r
    up = jnp.logical_and(q >= r, has_above)
    down = jnp.logical_and(q <= r, has_below)

    def columns(half, k):
        return pl.ds(pl.multiple_of(half * width + k * step, 128), step)

    def remote(src, k, send, recv, device):
        return pltpu.make_async_remote_copy(
            src_ref=src,
            dst_ref=out.at[:, columns(h, k)],
            send_sem=send.at[k],
            recv_sem=recv.at[k],
            device_id=device,
            device_id_type=MESH,
        )

    def send_all(src, k):
        @pl.when(up)
        def _():
            remote(src, k, far_send, far_recv, above).start()

        @pl.when(down)
        def _():
            remote(src, k, near_send, far_recv, below).start()

        remote(src, k, side_send, side_recv, partner).start()

    @pl.when(source)
    def _():
        for k in range(pieces):
            send_all(block.at[:, pl.ds(k * step, step)], k)
        out[:, pl.ds(pl.multiple_of(h * width, 128), width)] = block[...]

    @pl.when(jnp.logical_not(source))
    def _():
        for k in range(pieces):
            landed = out.at[:, columns(h, k)]
            remote(landed, k, side_send, far_recv, partner).wait_recv()
            send_all(landed, k)

    for k in range(pieces):
        mine = block.at[:, pl.ds(k * step, step)]

        @pl.when(up)
        def _():
            remote(mine, k, far_send, far_recv, above).wait_send()

        @pl.when(down)
        def _():
            remote(mine, k, near_send, far_recv, below).wait_send()

        remote(mine, k, side_send, side_recv, partner).wait_send()
        pltpu.make_async_remote_copy(
            src_ref=mine,
            dst_ref=out.at[:, columns(1 - h, k)],
            send_sem=side_send.at[k],
            recv_sem=side_recv.at[k],
            device_id=partner,
            device_id_type=MESH,
        ).wait_recv()


def spread(block, n_q, collective_id):
    maps, width = block.shape
    pieces = width // 128
    vmem = pl.BlockSpec(memory_space=pltpu.VMEM)
    sems = pltpu.SemaphoreType.DMA((pieces,))
    return pl.pallas_call(
        functools.partial(spread_kernel, n_q),
        out_shape=jax.ShapeDtypeStruct((maps, 2 * width), block.dtype),
        in_specs=[vmem],
        out_specs=vmem,
        scratch_shapes=[sems] * 5,
        compiler_params=pltpu.CompilerParams(
            collective_id=collective_id, has_side_effects=True
        ),
        name="spread%d" % collective_id,
    )(block)


def sum_kernel(n, place_of, device_of, x, out, landed, result, send1, recv1, send2, recv2):
    me = place_of()
    barrier = pltpu.get_barrier_semaphore()

    def each(body):
        lax.fori_loop(1, n, lambda k, carry: (body(k), carry)[1], 0)

    def member(k):
        return device_of(lax.rem(me + k, n))

    each(lambda k: pl.semaphore_signal(barrier, inc=1, device_id=member(k), device_id_type=MESH))
    pl.semaphore_wait(barrier, n - 1)

    def scatter(k):
        return pltpu.make_async_remote_copy(
            src_ref=x.at[lax.rem(me + k, n)],
            dst_ref=landed.at[k - 1],
            send_sem=send1.at[k - 1],
            recv_sem=recv1.at[k - 1],
            device_id=member(k),
            device_id_type=MESH,
        )

    def gather(k, slot):
        return pltpu.make_async_remote_copy(
            src_ref=result,
            dst_ref=out.at[slot],
            send_sem=send2.at[k - 1],
            recv_sem=recv2.at[k - 1],
            device_id=member(k),
            device_id_type=MESH,
        )

    each(lambda k: scatter(k).start())
    each(lambda k: scatter(k).wait_recv())
    total = lax.fori_loop(0, n - 1, lambda k, t: t + landed[k], x[me]) if n > 8 else sum(
        (landed[k] for k in range(n - 1)), x[me]
    )
    result[...] = total.astype(result.dtype)
    each(lambda k: gather(k, me).start())
    out[me] = result[...]
    each(lambda k: gather(k, lax.rem(me - k + n, n)).wait_recv())
    each(lambda k: scatter(k).wait_send())
    each(lambda k: gather(k, me).wait_send())


def pair_kernel(
    n, place_of, device_of, x, out, from_pair, pair_sum, landed, result,
    send1, recv1, send2, recv2, send3, recv3, send4, recv4,
):
    me = place_of()
    m = n // 2
    side, spot = me % 2, me // 2
    partner = device_of(me + 1 - 2 * side)

    def member(k):
        return device_of(lax.rem(spot + k, m) * 2 + side)

    def copy(src, dst, send, recv, device):
        return pltpu.make_async_remote_copy(
            src_ref=src, dst_ref=dst, send_sem=send, recv_sem=recv,
            device_id=device, device_id_type=MESH,
        )

    def first(k):
        j = lax.rem(spot + k, m)
        return copy(x.at[2 * j + 1 - side], from_pair.at[j], send1.at[k - 1], recv1.at[k - 1], partner)

    def second(k):
        return copy(pair_sum.at[k - 1], landed.at[k - 1], send2.at[k - 1], recv2.at[k - 1], member(k))

    def third(k, slot):
        return copy(result, out.at[slot], send3.at[k - 1], recv3.at[k - 1], member(k))

    def fourth(k, parity):
        slot = lax.rem(spot - k + m, m) * 2 + parity
        src = result if k == 0 else out.at[slot]
        return copy(src, out.at[slot], send4.at[k], recv4.at[k], partner)

    barrier = pltpu.get_barrier_semaphore()
    pl.semaphore_signal(barrier, inc=1, device_id=partner, device_id_type=MESH)
    for k in range(1, m):
        pl.semaphore_signal(barrier, inc=1, device_id=member(k), device_id_type=MESH)
    pl.semaphore_wait(barrier, m)
    for k in range(1, m + 1):
        first(k).start()
    for k in range(1, m):
        j = lax.rem(spot + k, m)
        first(k).wait_recv()
        pair_sum[k - 1] = x[2 * j + side] + from_pair[j]
        second(k).start()
    first(m).wait_recv()
    total = x[me] + from_pair[spot]
    for k in range(1, m):
        second(k).wait_recv()
        total = total + landed[k - 1]
    result[...] = total.astype(result.dtype)
    for k in range(1, m):
        third(k, me).start()
    fourth(0, side).start()
    out[me] = result[...]
    for k in range(1, m):
        third(k, lax.rem(spot - k + m, m) * 2 + side).wait_recv()
        fourth(k, side).start()
    for k in range(m):
        fourth(k, 1 - side).wait_recv()
    for k in range(1, m + 1):
        first(k).wait_send()
    for k in range(1, m):
        second(k).wait_send()
        third(k, me).wait_send()
    for k in range(m):
        fourth(k, side).wait_send()


def pair_sum_and_share(x, dtype, place_of, device_of, collective_id):
    n, rows, cols = x.shape
    m = n // 2
    vmem = pl.BlockSpec(memory_space=pltpu.VMEM)
    whole, rest = pltpu.SemaphoreType.DMA((m,)), pltpu.SemaphoreType.DMA((m - 1,))
    return pl.pallas_call(
        functools.partial(pair_kernel, n, place_of, device_of),
        out_shape=jax.ShapeDtypeStruct(x.shape, dtype),
        in_specs=[vmem],
        out_specs=vmem,
        scratch_shapes=[
            pltpu.VMEM((m, rows, cols), x.dtype),
            pltpu.VMEM((m - 1, rows, cols), x.dtype),
            pltpu.VMEM((m - 1, rows, cols), x.dtype),
            pltpu.VMEM((rows, cols), dtype),
            whole, whole, rest, rest, rest, rest, whole, whole,
        ],
        compiler_params=pltpu.CompilerParams(
            collective_id=collective_id, has_side_effects=True
        ),
        name="sum%d" % collective_id,
    )(x)


def sum_and_share(x, dtype, place_of, device_of, collective_id):
    n, rows, cols = x.shape
    vmem = pl.BlockSpec(memory_space=pltpu.VMEM)
    sems = pltpu.SemaphoreType.DMA((n - 1,))
    return pl.pallas_call(
        functools.partial(sum_kernel, n, place_of, device_of),
        out_shape=jax.ShapeDtypeStruct(x.shape, dtype),
        in_specs=[vmem],
        out_specs=vmem,
        scratch_shapes=[
            pltpu.VMEM((n - 1, rows, cols), x.dtype),
            pltpu.VMEM((rows, cols), dtype),
            sems, sems, sems, sems,
        ],
        compiler_params=pltpu.CompilerParams(
            collective_id=collective_id, has_side_effects=True
        ),
        name="sum%d" % collective_id,
    )(x)


def per_device(npix, n_rows, n_cols, inverse_cov, cosines, sky_maps):
    maps = sky_maps.shape[1]
    cols_here = inverse_cov.shape[1]
    n_q = n_cols // 2
    sky_rows = spread(sky_maps.T, n_q, 1)
    partial_value = jnp.dot(sky_rows, inverse_cov, preferred_element_type=jnp.float32)
    column_maps = pair_sum_and_share(
        partial_value.reshape(n_rows, maps // n_rows, cols_here),
        jnp.bfloat16,
        lambda: lax.axis_index("prow"),
        lambda i: (i, lax.axis_index("pcol")),
        2,
    ).reshape(maps, cols_here)
    row_maps = spread(column_maps, n_q, 3)
    moments = spectra_moments(cosines, row_maps, column_maps)
    devices = n_rows * n_cols
    matrix, each = transform_matrix(npix, devices)
    partial_spectra = jnp.dot(jnp.asarray(matrix), moments, precision=lax.Precision.HIGHEST)
    shared = sum_and_share(
        partial_spectra.reshape(devices, each, maps),
        jnp.float32,
        lambda: lax.axis_index("prow") * n_cols + lax.axis_index("pcol"),
        lambda i: (i // n_cols, lax.rem(i, n_cols)),
        4,
    )
    spectra = shared.reshape(devices * each, maps)[:L]
    return (row_maps.T, spectra)


def solution(mesh):
    in_specs = (P("prow", "pcol"), P("prow", "pcol"), P("pcol", None))
    out_specs = (P("prow", None), P())
    n_rows, n_cols = mesh.shape["prow"], mesh.shape["pcol"]

    def whole(inverse_cov, cosines, sky_maps):
        npix = cosines.shape[0]
        step = jax.shard_map(
            functools.partial(per_device, npix, n_rows, n_cols),
            mesh=mesh, in_specs=in_specs, out_specs=out_specs, check_vma=False,
        )
        return step(inverse_cov, cosines, sky_maps)

    return whole
```

```python
import functools
import math
import random

import jax
import jax.numpy as jnp
import numpy as np
from jax import lax
from jax.experimental import pallas as pl
from jax.experimental.pallas import tpu as pltpu
from jax.sharding import PartitionSpec as P

L = 64
LMIN = 2
TILE = 256
STRIP = 16
LOW = 11
HIGH = 6
LEVELS = LOW * HIGH


def transform_matrix(npix, devices):
    top = LMIN + L - 1
    each = -(-L // devices)
    a = [math.comb(2 * k, k) / 4.0**k for k in range(top + 1)]
    product = np.zeros((LEVELS, LEVELS))
    for k in range(LEVELS):
        high, low = divmod(k, LOW)
        product[k, low * HIGH + high] = 1
        if high and low:
            product[k, low * HIGH + high] = 2
            product[k] -= product[high * LOW - low]
    out = np.zeros((devices * each, LEVELS))
    for l in range(LMIN, top + 1):
        owner, place = divmod(l - LMIN, each)
        row = out[owner * each + place]
        for k in range(l + 1):
            row[abs(l - 2 * k)] += a[k] * a[l - k]
        row *= (2 * l + 1) / npix
    return (out @ product).astype(np.float32), each


def pair_up(tiles, n):
    items = []
    for col in range(n):
        mine = sorted((t for t in tiles if t[1] == col), key=lambda t: t[0])
        for k in range(0, len(mine), 2):
            first = mine[k]
            second = mine[k + 1] if k + 1 < len(mine) else (first[0], col, 0)
            items.append((first[0], second[0], first[2], second[2], col))
    return items


def work_tables(n):
    lower = [[(h * n + i, j, 2) for i in range(n) for j in range(n)] for h in range(2)]
    rng = random.Random(0)
    best = None
    for _ in range(20000):
        sets = []
        cross = [[rng.random() < 0.5 for _ in range(n)] for _ in range(n)]
        for h in range(2):
            tiles = []
            for i in range(n):
                tiles.append((h * n + i, i, 1))
                for j in range(i):
                    a, b = (i, j) if rng.random() < 0.5 else (j, i)
                    tiles.append((h * n + a, b, 2))
                for j in range(n):
                    if h == 0 and cross[i][j]:
                        tiles.append((n + i, j, 2))
                    if h == 1 and not cross[i][j]:
                        tiles.append((j, i, 2))
            sets.append(pair_up(tiles, n))
        cost = max(len(s) for s in sets)
        if best is None or cost < best[0]:
            best = (cost, sets)
        if 2 * cost <= n * n + n // 2 + 1:
            break
    kinds = [pair_up(lower[0], n), pair_up(lower[1], n), pair_up(lower[1], n), pair_up(lower[0], n)] + best[1]
    longest = max(len(k) for k in kinds)
    table = np.zeros((len(kinds), longest + 1, 5), np.int32)
    for k, items in enumerate(kinds):
        table[k, : len(items)] = items
    counts = np.array([len(k) for k in kinds], np.int32)
    return table.reshape(-1), counts, longest + 1


def moments_kernel(
    stride, longest, table, counts, cos_hbm, ft, fct, out,
    xbuf, buf_a, buf_b, lhs, fj, acc, sem,
):
    r = lax.axis_index("prow")
    c = lax.axis_index("pcol")
    q, h = c // 2, c % 2
    kind = jnp.where(r > q, h, jnp.where(r < q, 2 + h, 4 + h))
    n_items = counts[kind]
    n_strips = 2 * TILE // STRIP

    def field(item, f):
        return table[(kind * stride + item) * 5 + f]

    def tile_copy(item, half):
        row = pl.multiple_of(field(item, half) * TILE, TILE)
        col = pl.multiple_of(field(item, 4) * TILE, TILE)
        return pltpu.make_async_copy(
            cos_hbm.at[pl.ds(row, TILE), pl.ds(col, TILE)],
            xbuf.at[item, pl.ds(half * TILE, TILE)],
            sem.at[item, half],
        )

    def fetch(item, carry):
        tile_copy(item, 0).start()
        tile_copy(item, 1).start()
        return carry

    def landed(item):
        @pl.when(item < n_items)
        def _():
            tile_copy(item, 0).wait()
            tile_copy(item, 1).wait()

    def set_operands(item):
        col = pl.multiple_of(field(item, 4) * TILE, TILE)
        for half in range(2):
            row = pl.multiple_of(field(item, half) * TILE, TILE)
            weight = field(item, 2 + half).astype(jnp.float32)
            value = ft[:, pl.ds(row, TILE)].astype(jnp.float32) * weight
            lhs[:, half * TILE : (half + 1) * TILE] = value.astype(jnp.bfloat16)
        fj[...] = fct[:, pl.ds(col, TILE)].astype(jnp.float32)

    def gen_strip(buf, item, s):
        rows = pl.ds(pl.multiple_of(s * STRIP, STRIP), STRIP)
        x = xbuf[item, rows, :]
        xx = x + x
        buf[1, rows, :] = x.astype(jnp.bfloat16)
        p, t = x, xx * x - 1.0
        for k in range(2, LOW):
            buf[k, rows, :] = t.astype(jnp.bfloat16)
            p, t = t, xx * t - p
        yy = t + t
        buf[LOW, rows, :] = t.astype(jnp.bfloat16)
        p, t = t, yy * t - 1.0
        for k in range(2, HIGH):
            buf[LOW + k - 1, rows, :] = t.astype(jnp.bfloat16)
            p, t = t, yy * t - p

    def item_pass(item, use, gen):
        following = jnp.minimum(item + 1, n_items - 1)
        landed(item + 1)
        set_operands(item)

        half_tile = TILE // 2
        done = 0
        for level in range(LEVELS):
            k, g = divmod(level, HIGH)
            upto = (level + 1) * n_strips // LEVELS
            for s in range(done, upto):
                gen_strip(gen, following, s)
            done = upto
            if k == 0:
                rhs = use[LOW + g - 1] if g else use[0]
            else:
                rhs = use[LOW + g - 1] * use[k] if g else use[k]
            image = jnp.dot(lhs[...], rhs, preferred_element_type=jnp.float32)
            prod = image * fj[...]
            folded = prod[:, :half_tile] + prod[:, half_tile:]
            acc[level] += folded
            xbuf[longest, 0:8, 0:half_tile] = folded[0:8, :]

    lax.fori_loop(0, n_items, fetch, 0)
    acc[...] = jnp.zeros_like(acc)
    for buf in (buf_a, buf_b):
        buf[0] = jnp.ones(buf.shape[1:], buf.dtype)
    landed(0)

    def first(s, carry):
        gen_strip(buf_a, 0, s)
        return carry

    lax.fori_loop(0, n_strips, first, 0, unroll=4)

    def two_items(pair, carry):
        item_pass(2 * pair, buf_a, buf_b)

        @pl.when(2 * pair + 1 < n_items)
        def _():
            item_pass(2 * pair + 1, buf_b, buf_a)

        return carry

    lax.fori_loop(0, (n_items + 1) // 2, two_items, 0)
    out[...] = jnp.sum(acc[...], axis=-1)


def spectra_moments(cosines, ft, fct):
    maps = ft.shape[0]
    n = cosines.shape[1] // TILE
    table, counts, stride = work_tables(n)
    longest = int(counts.max())
    vmem = pl.BlockSpec(memory_space=pltpu.VMEM)
    smem = pl.BlockSpec(memory_space=pltpu.SMEM)
    return pl.pallas_call(
        functools.partial(moments_kernel, stride, longest),
        out_shape=jax.ShapeDtypeStruct((LEVELS, maps), jnp.float32),
        in_specs=[smem, smem, pl.BlockSpec(memory_space=pl.ANY), vmem, vmem],
        out_specs=vmem,
        scratch_shapes=[
            pltpu.VMEM((longest + 1, 2 * TILE, TILE), jnp.float32),
            pltpu.VMEM((LOW + HIGH - 1, 2 * TILE, TILE), jnp.bfloat16),
            pltpu.VMEM((LOW + HIGH - 1, 2 * TILE, TILE), jnp.bfloat16),
            pltpu.VMEM((maps, 2 * TILE), jnp.bfloat16),
            pltpu.VMEM((maps, TILE), jnp.float32),
            pltpu.VMEM((LEVELS, maps, TILE // 2), jnp.float32),
            pltpu.SemaphoreType.DMA((longest, 2)),
        ],
        compiler_params=pltpu.CompilerParams(vmem_limit_bytes=48 * 2**20),
        name="moments",
    )(jnp.asarray(table), jnp.asarray(counts), cosines, ft, fct)


MESH = pl.DeviceIdType.MESH
CHUNKS = 4


def weigh_kernel(
    n_rows, n_q, sky, cov_hbm, ft, fct,
    cov, x_out, x_in, mine, z_out, z_in,
    cov_sem, x_send, x_recv, z_send, z_recv, a_send, a_recv, p_send, p_recv, c_send, c_recv,
):
    r = lax.axis_index("prow")
    c = lax.axis_index("pcol")
    q, h = c // 2, c % 2
    maps = sky.shape[0]
    group = maps // n_q
    half = cov.shape[0] // 2
    width = half // CHUNKS
    partner = (r, c + 1 - 2 * h)
    diagonal = r == q

    def line(k):
        return lax.rem(q + k, n_q)

    def other(k):
        return lax.rem(r + k, n_rows)

    def at(j):
        return pl.ds(j * width, width)

    def placed(j):
        return pl.ds(pl.multiple_of(h * half + j * width, width), width)

    def cov_copy(j, own):
        side = h if own else 1 - h
        return pltpu.make_async_copy(
            cov_hbm.at[pl.ds(pl.multiple_of(side * half + j * width, width), width)],
            cov.at[pl.ds((int(own) * CHUNKS + j) * width, width)],
            cov_sem.at[int(own) * CHUNKS + j],
        )

    def copy(src, dst, send, recv, device):
        return pltpu.make_async_remote_copy(
            src_ref=src, dst_ref=dst, send_sem=send, recv_sem=recv,
            device_id=device, device_id_type=MESH,
        )

    def x_copy(j):
        return copy(x_out.at[j], x_in.at[j], x_send.at[j], x_recv.at[j], partner)

    def z_copy(j, k):
        return copy(
            z_out.at[line(k), :, at(j)], z_in.at[k - 1, :, at(j)],
            z_send.at[j, k - 1], z_recv.at[j, k - 1], (r, line(k) * 2 + h),
        )

    def a_copy(j, k):
        return copy(
            ft.at[q, :, placed(j)], ft.at[q, :, placed(j)],
            a_send.at[j, k - 1], a_recv.at[j, k - 1], (r, line(k) * 2 + h),
        )

    def a_arrival(j, k):
        g = line(n_q - k)
        return g, copy(
            ft.at[g, :, placed(j)], ft.at[g, :, placed(j)],
            a_send.at[j, k - 1], a_recv.at[j, k - 1], partner,
        )

    def p_copy(j, g, slot):
        return copy(
            ft.at[g, :, placed(j)], ft.at[g, :, placed(j)],
            p_send.at[j, slot], p_recv.at[j, slot], partner,
        )

    def c_copy(j, g, slot, k):
        return copy(
            ft.at[g, :, placed(j)], fct.at[g, :, at(j)],
            c_send.at[j, slot, k - 1], c_recv.at[j, slot], (other(k), c),
        )

    def product(j, own):
        cov_copy(j, own).wait()
        block = cov[(int(own) * CHUNKS + j) * width : (int(own) * CHUNKS + j + 1) * width, :]
        return lax.dot_general(
            sky[...], block, (((1,), (1,)), ((), ())), preferred_element_type=jnp.float32
        )

    def share(j, g, slot):
        @pl.when(diagonal)
        def _():
            for k in range(1, n_rows):
                c_copy(j, g, slot, k).start()

        p_copy(j, g, slot).start()

    for own in (False, True):
        for j in range(CHUNKS):
            cov_copy(j, own).start()
    barrier = pltpu.get_barrier_semaphore()
    greeted = [partner]
    greeted += [(r, line(k) * 2 + h) for k in range(1, n_q)]
    greeted += [(other(k), c) for k in range(1, n_rows)]
    for device in greeted:
        pl.semaphore_signal(barrier, inc=1, device_id=device, device_id_type=MESH)
    for j in range(CHUNKS):
        x_out[j] = product(j, False).astype(x_out.dtype)
        if j == 0:
            pl.semaphore_wait(barrier, len(greeted))
        x_copy(j).start()
    for j in range(CHUNKS):
        total = product(j, True)
        for g in range(n_q):
            mine[g, :, j * width : (j + 1) * width] = total[g * group : (g + 1) * group]
    for j in range(CHUNKS):
        x_copy(j).wait_recv()
        for g in range(n_q):
            total = mine[g, :, j * width : (j + 1) * width] + x_in[j, g * group : (g + 1) * group]
            mine[g, :, j * width : (j + 1) * width] = total
            z_out[g, :, j * width : (j + 1) * width] = total.astype(z_out.dtype)
        for k in range(1, n_q):
            z_copy(j, k).start()
    lag = min(2, CHUNKS)
    for step in range(CHUNKS + lag):
        if step < CHUNKS:
            j = step
            total = mine[q, :, j * width : (j + 1) * width]
            for k in range(1, n_q):
                z_copy(j, k).wait_recv()
                total = total + z_in[k - 1, :, j * width : (j + 1) * width]
            ft[q, :, placed(j)] = total.astype(ft.dtype)
            for k in range(1, n_q):
                a_copy(j, k).start()
            share(j, q, 0)
        if step >= lag:
            j = step - lag
            for k in range(1, n_q):
                g, arrival = a_arrival(j, k)
                arrival.wait_recv()
                share(j, g, k)

    def mirrored(slot):
        return q if slot == 0 else line(n_q - slot)

    @pl.when(diagonal)
    def _():
        fct[...] = ft[:, :, pl.ds(pl.multiple_of(h * half, half), half)]
        for j in range(CHUNKS):
            for slot in range(n_q):
                for k in range(1, n_rows):
                    c_copy(j, mirrored(slot), slot, k).wait_send()

    @pl.when(jnp.logical_not(diagonal))
    def _():
        for j in range(CHUNKS):
            for slot in range(n_q):
                copy(
                    ft.at[q, :, placed(j)], fct.at[mirrored(slot), :, at(j)],
                    c_send.at[j, slot, 0], c_recv.at[j, slot], partner,
                ).wait_recv()

    for j in range(CHUNKS):
        x_copy(j).wait_send()
        for k in range(1, n_q):
            z_copy(j, k).wait_send()
            a_copy(j, k).wait_send()
        for slot in range(n_q):
            g = mirrored(slot)
            outward = p_copy(j, g, slot)
            outward.wait_send()
            elsewhere = pl.ds(pl.multiple_of((1 - h) * half + j * width, width), width)
            copy(
                ft.at[g, :, elsewhere], ft.at[g, :, elsewhere],
                p_send.at[j, slot], p_recv.at[j, slot], partner,
            ).wait_recv()


def weigh(sky, cov, n_rows, n_q):
    maps, depth = sky.shape
    rows = cov.shape[0]
    half = rows // 2
    width = half // CHUNKS
    group = maps // n_q
    vmem = pl.BlockSpec(memory_space=pltpu.VMEM)
    dma = pltpu.SemaphoreType.DMA
    return pl.pallas_call(
        functools.partial(weigh_kernel, n_rows, n_q),
        out_shape=[
            jax.ShapeDtypeStruct((n_q, group, rows), jnp.bfloat16),
            jax.ShapeDtypeStruct((n_q, group, half), jnp.bfloat16),
        ],
        in_specs=[vmem, pl.BlockSpec(memory_space=pl.ANY)],
        out_specs=[vmem, vmem],
        scratch_shapes=[
            pltpu.VMEM((rows, depth), jnp.bfloat16),
            pltpu.VMEM((CHUNKS, maps, width), jnp.bfloat16),
            pltpu.VMEM((CHUNKS, maps, width), jnp.bfloat16),
            pltpu.VMEM((n_q, group, half), jnp.float32),
            pltpu.VMEM((n_q, group, half), jnp.bfloat16),
            pltpu.VMEM((n_q - 1, group, half), jnp.bfloat16),
            dma((2 * CHUNKS,)),
            dma((CHUNKS,)), dma((CHUNKS,)),
            dma((CHUNKS, n_q - 1)), dma((CHUNKS, n_q - 1)),
            dma((CHUNKS, n_q - 1)), dma((CHUNKS, n_q - 1)),
            dma((CHUNKS, n_q)), dma((CHUNKS, n_q)),
            dma((CHUNKS, n_q, n_rows - 1)), dma((CHUNKS, n_q)),
        ],
        compiler_params=pltpu.CompilerParams(
            collective_id=1, has_side_effects=True, vmem_limit_bytes=32 * 2**20
        ),
        name="weigh",
    )(sky, cov)


def sum_kernel(n, place_of, device_of, x, out, landed, result, send1, recv1, send2, recv2):
    me = place_of()
    barrier = pltpu.get_barrier_semaphore()

    def each(body):
        lax.fori_loop(1, n, lambda k, carry: (body(k), carry)[1], 0)

    def member(k):
        return device_of(lax.rem(me + k, n))

    each(lambda k: pl.semaphore_signal(barrier, inc=1, device_id=member(k), device_id_type=MESH))
    pl.semaphore_wait(barrier, n - 1)

    def scatter(k):
        return pltpu.make_async_remote_copy(
            src_ref=x.at[lax.rem(me + k, n)],
            dst_ref=landed.at[k - 1],
            send_sem=send1.at[k - 1],
            recv_sem=recv1.at[k - 1],
            device_id=member(k),
            device_id_type=MESH,
        )

    def gather(k, slot):
        return pltpu.make_async_remote_copy(
            src_ref=result,
            dst_ref=out.at[slot],
            send_sem=send2.at[k - 1],
            recv_sem=recv2.at[k - 1],
            device_id=member(k),
            device_id_type=MESH,
        )

    each(lambda k: scatter(k).start())
    each(lambda k: scatter(k).wait_recv())
    total = lax.fori_loop(0, n - 1, lambda k, t: t + landed[k], x[me]) if n > 8 else sum(
        (landed[k] for k in range(n - 1)), x[me]
    )
    result[...] = total.astype(result.dtype)
    each(lambda k: gather(k, me).start())
    out[me] = result[...]
    each(lambda k: gather(k, lax.rem(me - k + n, n)).wait_recv())
    each(lambda k: scatter(k).wait_send())
    each(lambda k: gather(k, me).wait_send())


def sum_and_share(x, dtype, place_of, device_of, collective_id):
    n, rows, cols = x.shape
    vmem = pl.BlockSpec(memory_space=pltpu.VMEM)
    sems = pltpu.SemaphoreType.DMA((n - 1,))
    return pl.pallas_call(
        functools.partial(sum_kernel, n, place_of, device_of),
        out_shape=jax.ShapeDtypeStruct(x.shape, dtype),
        in_specs=[vmem],
        out_specs=vmem,
        scratch_shapes=[
            pltpu.VMEM((n - 1, rows, cols), x.dtype),
            pltpu.VMEM((rows, cols), dtype),
            sems, sems, sems, sems,
        ],
        compiler_params=pltpu.CompilerParams(
            collective_id=collective_id, has_side_effects=True
        ),
        name="sum%d" % collective_id,
    )(x)


def per_device(npix, n_rows, n_cols, inverse_cov, cosines, sky_maps):
    maps = sky_maps.shape[1]
    n_q = n_cols // 2
    ft, fct = weigh(sky_maps.T, inverse_cov, n_rows, n_q)
    row_maps = ft.reshape(maps, ft.shape[2])
    column_maps = fct.reshape(maps, fct.shape[2])
    moments = spectra_moments(cosines, row_maps, column_maps)
    devices = n_rows * n_cols
    matrix, each = transform_matrix(npix, devices)
    partial_spectra = jnp.dot(jnp.asarray(matrix), moments, precision=lax.Precision.HIGHEST)
    shared = sum_and_share(
        partial_spectra.reshape(devices, each, maps),
        jnp.float32,
        lambda: lax.axis_index("prow") * n_cols + lax.axis_index("pcol"),
        lambda i: (i // n_cols, lax.rem(i, n_cols)),
        4,
    )
    spectra = shared.reshape(devices * each, maps)[:L]
    return (row_maps.T, spectra)


def solution(mesh):
    in_specs = (P("prow", "pcol"), P("prow", "pcol"), P("pcol", None))
    out_specs = (P("prow", None), P())
    n_rows, n_cols = mesh.shape["prow"], mesh.shape["pcol"]

    def whole(inverse_cov, cosines, sky_maps):
        npix = cosines.shape[0]
        step = jax.shard_map(
            functools.partial(per_device, npix, n_rows, n_cols),
            mesh=mesh, in_specs=in_specs, out_specs=out_specs, check_vma=False,
        )
        return step(inverse_cov, cosines, sky_maps)

    return whole
```

```python
import functools
import math

import jax
import jax.numpy as jnp
import numpy as np
from jax import lax
from jax.experimental import pallas as pl
from jax.experimental.pallas import tpu as pltpu
from jax.sharding import PartitionSpec as P

L = 64
LMIN = 2
TILE = 256
STRIP = 16
LOW = 11
HIGH = 6
LEVELS = LOW * HIGH
FIELD = 64
MESH = pl.DeviceIdType.MESH


def transform_matrix(npix, devices):
    top = LMIN + L - 1
    each = -(-L // devices)
    a = [math.comb(2 * k, k) / 4.0**k for k in range(top + 1)]
    product = np.zeros((LEVELS, LEVELS))
    for k in range(LEVELS):
        high, low = divmod(k, LOW)
        product[k, low * HIGH + high] = 1
        if high and low:
            product[k, low * HIGH + high] = 2
            product[k] -= product[high * LOW - low]
    out = np.zeros((devices * each, LEVELS))
    for l in range(LMIN, top + 1):
        owner, place = divmod(l - LMIN, each)
        row = out[owner * each + place]
        for k in range(l + 1):
            row[abs(l - 2 * k)] += a[k] * a[l - k]
        row *= (2 * l + 1) / npix
    return (out @ product).astype(np.float32), each


def pair_up(tiles, n):
    items = []
    for col in range(n):
        mine = sorted((t for t in tiles if t[1] == col), key=lambda t: t[0])
        for k in range(0, len(mine), 2):
            first = mine[k]
            second = mine[k + 1] if k + 1 < len(mine) else (first[0], col, 0)
            items.append((first[0], second[0], first[2], second[2], col))
    return items


def work_tables(n):
    lower = [pair_up([(h * n + i, j, 2) for i in range(n) for j in range(n)], n) for h in range(2)]
    own = [(j, j, 1) for j in range(n)] + [(i, 0, 2) for i in range(1, n)]
    if n % 2:
        own += [(i, j, 2) for j in range(1, n) for i in range(j + 1, n)]
    else:
        own += [
            (1 + (j - 1 + d) % (n - 1), j, 2)
            for j in range(1, n) for d in range(1, n // 2)
        ]
    kinds, needed = [], []
    for h in range(2):
        kinds.append(lower[h])
        needed.append(-1)
    for h in range(2):
        kinds.append(lower[1 - h])
        needed.append(0)
    for h in range(2):
        near = pair_up([(h * n + i, j, w) for i, j, w in own], n)
        far = [
            ((1 - h) * n + i, j, 2)
            for i in range(n) for j in range(n) if (i + j) % 2 == h
        ]
        kinds.append(near + pair_up(far, n))
        needed.append(len(near))
    longest = max(len(k) for k in kinds)
    codes = [
        [row0 + FIELD * (row1 + FIELD * (w0 + FIELD * (w1 + FIELD * col))) for row0, row1, w0, w1, col in k]
        for k in kinds
    ]
    return codes, needed, longest


def spectra_kernel(
    n_rows, n_q, codes, needed, longest, sky_hbm, cov_hbm, cos_hbm, matrix_hbm, weighed, out,
    sky, matrix, cov, x_out, x_in, mine, z_out, z_in, ft, fct, xbuf, buf_a, buf_b, lhs, fj, acc,
    sums, parts, landing, summed, shared,
    in_sem, cov_sem, x_send, x_recv, z_send, z_recv, a_send, a_recv, p_send, p_recv, c_send, c_recv,
    tile_sem, s_send, s_recv, g_send, g_recv, row_ready, all_ready,
):
    r = lax.axis_index("prow")
    c = lax.axis_index("pcol")
    q, h = c // 2, c % 2
    maps = sky.shape[0]
    devices = parts.shape[0]
    each = parts.shape[1]
    me = r * (2 * n_q) + c
    group = maps // n_q
    half = cov.shape[0] // 2
    chunks, width = x_out.shape[0], x_out.shape[2]
    partner = (r, c + 1 - 2 * h)
    diagonal = r == q

    def line(k):
        return lax.rem(q + k, n_q)

    def other(k):
        return lax.rem(r + k, n_rows)

    def placed(j):
        return h * chunks + j

    def cov_copy(j, own):
        side = h if own else 1 - h
        return pltpu.make_async_copy(
            cov_hbm.at[pl.ds(pl.multiple_of(side * half + j * width, width), width)],
            cov.at[pl.ds((int(own) * chunks + j) * width, width)],
            cov_sem.at[int(own) * chunks + j],
        )

    def copy(src, dst, send, recv, device):
        return pltpu.make_async_remote_copy(
            src_ref=src, dst_ref=dst, send_sem=send, recv_sem=recv,
            device_id=device, device_id_type=MESH,
        )

    def x_copy(j):
        return copy(x_out.at[j], x_in.at[j], x_send.at[j], x_recv.at[j], partner)

    def z_copy(j, k):
        return copy(
            z_out.at[j, line(k)], z_in.at[j, k - 1],
            z_send.at[j, k - 1], z_recv.at[j, k - 1], (r, line(k) * 2 + h),
        )

    def a_copy(j, k):
        return copy(
            ft.at[placed(j), q], ft.at[placed(j), q],
            a_send.at[j, k - 1], a_recv.at[j, k - 1], (r, line(k) * 2 + h),
        )

    def a_arrival(j, k):
        g = line(n_q - k)
        return g, copy(
            ft.at[placed(j), g], ft.at[placed(j), g],
            a_send.at[j, k - 1], a_recv.at[j, k - 1], partner,
        )

    def p_copy(j, g, slot):
        return copy(
            ft.at[placed(j), g], ft.at[placed(j), g],
            p_send.at[j, slot], p_recv.at[j, slot], partner,
        )

    def c_copy(j, g, slot, k):
        return copy(
            ft.at[placed(j), g], fct.at[j, g],
            c_send.at[j, slot, k - 1], c_recv.at[j, slot], (other(k), c),
        )

    def product(j, own):
        cov_copy(j, own).wait()
        block = cov[(int(own) * chunks + j) * width : (int(own) * chunks + j + 1) * width, :]
        return lax.dot_general(
            sky[...], block, (((1,), (1,)), ((), ())), preferred_element_type=jnp.float32
        )

    def share(j, g, slot):
        @pl.when(diagonal)
        def _():
            for k in range(1, n_rows):
                c_copy(j, g, slot, k).start()

        p_copy(j, g, slot).start()

    kind = jnp.where(r > q, h, jnp.where(r < q, 2 + h, 4 + h))
    n_strips = 2 * TILE // STRIP

    def by_kind(values):
        chosen = jnp.int32(values[0])
        for i in range(1, len(values)):
            chosen = jnp.where(kind == i, jnp.int32(values[i]), chosen)
        return chosen

    n_items = by_kind([len(k) for k in codes])
    other_from = by_kind(needed)
    item_codes = [by_kind([k[i] if i < len(k) else k[0] for k in codes]) for i in range(longest)]

    def fields(item):
        code = item_codes[0]
        for i in range(1, longest):
            code = jnp.where(item == i, item_codes[i], code)
        found = []
        for _ in range(5):
            found.append(code % FIELD)
            code = code // FIELD
        return found

    def tile_copies(item):
        row0, row1, _, _, col = fields(item)
        for side, row in enumerate((row0, row1)):
            yield pltpu.make_async_copy(
                cos_hbm.at[
                    pl.ds(pl.multiple_of(row * TILE, TILE), TILE),
                    pl.ds(pl.multiple_of(col * TILE, TILE), TILE),
                ],
                xbuf.at[item, pl.ds(side * TILE, TILE)],
                tile_sem.at[item, side],
            )

    def fetch(item, carry):
        for tile in tile_copies(item):
            tile.start()
        return carry

    def landed(item):
        @pl.when(item < n_items)
        def _():
            for tile in tile_copies(item):
                tile.wait()

    def set_operands(item):
        row0, row1, w0, w1, col = fields(item)
        for side, (row, weight) in enumerate(((row0, w0), (row1, w1))):
            value = [ft[row, g].astype(jnp.float32) for g in range(n_q)]
            value = jnp.concatenate(value, axis=0) * weight.astype(jnp.float32)
            lhs[:, side * TILE : (side + 1) * TILE] = value.astype(jnp.bfloat16)
        for g in range(n_q):
            fj[g * group : (g + 1) * group] = fct[col, g].astype(jnp.float32)

    def gen_strip(buf, item, s):
        rows = pl.ds(pl.multiple_of(s * STRIP, STRIP), STRIP)
        x = xbuf[item, rows, :]
        xx = x + x
        buf[1, rows, :] = x.astype(jnp.bfloat16)
        p, t = x, xx * x - 1.0
        for k in range(2, LOW):
            buf[k, rows, :] = t.astype(jnp.bfloat16)
            p, t = t, xx * t - p
        yy = t + t
        buf[LOW, rows, :] = t.astype(jnp.bfloat16)
        p, t = t, yy * t - 1.0
        for k in range(2, HIGH):
            buf[LOW + k - 1, rows, :] = t.astype(jnp.bfloat16)
            p, t = t, yy * t - p

    def item_pass(item, use, gen):
        following = jnp.minimum(item + 1, n_items - 1)
        landed(item + 1)

        @pl.when(item == other_from)
        def _():
            other_half()

        set_operands(item)

        half_tile = TILE // 2
        done = 0
        for level in range(LEVELS):
            k, g = divmod(level, HIGH)
            upto = (level + 1) * n_strips // LEVELS
            for s in range(done, upto):
                gen_strip(gen, following, s)
            done = upto
            if k == 0:
                rhs = use[LOW + g - 1] if g else use[0]
            else:
                rhs = use[LOW + g - 1] * use[k] if g else use[k]
            image = jnp.dot(lhs[...], rhs, preferred_element_type=jnp.float32)
            prod = image * fj[...]
            folded = prod[:, :half_tile] + prod[:, half_tile:]
            acc[level] += folded
            xbuf[longest, 0:8, 0:half_tile] = folded[0:8, :]

    def first_strip(s, carry):
        gen_strip(buf_a, 0, s)
        return carry

    def two_items(pair, carry):
        item_pass(2 * pair, buf_a, buf_b)

        @pl.when(2 * pair + 1 < n_items)
        def _():
            item_pass(2 * pair + 1, buf_b, buf_a)

        return carry

    def member(k):
        device = lax.rem(me + k, devices)
        return (device // (2 * n_q), device % (2 * n_q))

    def each_other(body):
        lax.fori_loop(1, devices, lambda k, carry: (body(k), carry)[1], 0)

    def scatter(k):
        return copy(
            parts.at[lax.rem(me + k, devices)], landing.at[k - 1],
            s_send.at[k - 1], s_recv.at[k - 1], member(k),
        )

    def gather(k, slot):
        return copy(
            summed, shared.at[slot], g_send.at[k - 1], g_recv.at[k - 1], member(k)
        )

    def elsewhere(j, slot):
        g = mirrored(slot)
        where = (1 - h) * chunks + j
        return copy(
            ft.at[where, g], ft.at[where, g],
            p_send.at[j, slot], p_recv.at[j, slot], partner,
        )

    def other_half():
        for j in range(chunks):
            for slot in range(n_q):
                elsewhere(j, slot).wait_recv()

    def mirrored(slot):
        return q if slot == 0 else line(n_q - slot)

    sky_copy = pltpu.make_async_copy(sky_hbm, sky, in_sem.at[0])
    matrix_copy = pltpu.make_async_copy(matrix_hbm, matrix, in_sem.at[1])
    sky_copy.start()
    for own in (False, True):
        for j in range(chunks):
            cov_copy(j, own).start()
    matrix_copy.start()
    lax.fori_loop(0, n_items, fetch, 0)
    barrier = pltpu.get_barrier_semaphore()
    greeted = [partner]
    greeted += [(r, line(k) * 2 + h) for k in range(1, n_q)]
    greeted += [(other(k), c) for k in range(1, n_rows)]
    for device in greeted:
        pl.semaphore_signal(barrier, inc=1, device_id=device, device_id_type=MESH)
    sky_copy.wait()
    for j in range(chunks):
        x_out[j] = product(j, False).astype(x_out.dtype)
        if j == 0:
            pl.semaphore_wait(barrier, len(greeted))
            pl.semaphore_signal(row_ready, inc=1, device_id=partner, device_id_type=MESH)
        x_copy(j).start()
    for j in range(chunks):
        total = product(j, True)
        for g in range(n_q):
            mine[j, g] = total[g * group : (g + 1) * group]
    acc[...] = jnp.zeros_like(acc)
    for buf in (buf_a, buf_b):
        buf[0] = jnp.ones(buf.shape[1:], buf.dtype)
    landed(0)
    lax.fori_loop(0, n_strips, first_strip, 0, unroll=4)
    pl.semaphore_wait(row_ready, 1)
    for k in range(1, n_rows):
        pl.semaphore_signal(all_ready, inc=1, device_id=(other(k), c), device_id_type=MESH)
    for j in range(chunks):
        x_copy(j).wait_recv()
        for g in range(n_q):
            total = mine[j, g] + x_in[j, g * group : (g + 1) * group]
            mine[j, g] = total
            z_out[j, g] = total.astype(z_out.dtype)
        for k in range(1, n_q):
            z_copy(j, k).start()
    lag = min(2, chunks)
    for step in range(chunks + lag):
        if step < chunks:
            j = step
            total = mine[j, q]
            for k in range(1, n_q):
                z_copy(j, k).wait_recv()
                total = total + z_in[j, k - 1]
            ft[placed(j), q] = total.astype(ft.dtype)
            for k in range(1, n_q):
                a_copy(j, k).start()
            share(j, q, 0)
        if step >= lag:
            j = step - lag
            for k in range(1, n_q):
                g, arrival = a_arrival(j, k)
                arrival.wait_recv()
                share(j, g, k)

    @pl.when(diagonal)
    def _():
        for j in range(chunks):
            fct[j] = ft[placed(j)]

    @pl.when(jnp.logical_not(diagonal))
    def _():
        for j in range(chunks):
            for slot in range(n_q):
                copy(
                    ft.at[placed(j), q], fct.at[j, mirrored(slot)],
                    c_send.at[j, slot, 0], c_recv.at[j, slot], partner,
                ).wait_recv()

    lax.fori_loop(0, (n_items + 1) // 2, two_items, 0)
    sums[...] = jnp.zeros_like(sums)
    sums[0:LEVELS, :] = jnp.sum(acc[...], axis=-1)
    matrix_copy.wait()
    spectra = jnp.dot(
        matrix[...], sums[...],
        precision=lax.Precision.HIGHEST, preferred_element_type=jnp.float32,
    )
    for i in range(devices):
        parts[i] = spectra[i * each : (i + 1) * each]
    pl.semaphore_wait(all_ready, n_rows - 1)
    each_other(lambda k: scatter(k).start())

    @pl.when(r > q)
    def _():
        other_half()

    for t in range(2 * chunks):
        for g in range(n_q):
            weighed[g, :, t * width : (t + 1) * width] = ft[t, g]

    @pl.when(diagonal)
    def _():
        for j in range(chunks):
            for slot in range(n_q):
                for k in range(1, n_rows):
                    c_copy(j, mirrored(slot), slot, k).wait_send()

    for j in range(chunks):
        x_copy(j).wait_send()
        for k in range(1, n_q):
            z_copy(j, k).wait_send()
            a_copy(j, k).wait_send()
        for slot in range(n_q):
            p_copy(j, mirrored(slot), slot).wait_send()
    each_other(lambda k: scatter(k).wait_recv())
    summed[...] = lax.fori_loop(0, devices - 1, lambda k, t: t + landing[k], parts[me])
    each_other(lambda k: gather(k, me).start())
    shared[me] = summed[...]
    each_other(lambda k: gather(k, lax.rem(me - k + devices, devices)).wait_recv())
    for i in range(devices):
        if i * each < out.shape[0]:
            out[i * each : (i + 1) * each, :] = shared[i]
    each_other(lambda k: scatter(k).wait_send())
    each_other(lambda k: gather(k, me).wait_send())


def per_device(npix, n_rows, n_cols, inverse_cov, cosines, sky_maps):
    depth, maps = sky_maps.shape
    rows = inverse_cov.shape[0]
    n_q = n_cols // 2
    half, group = rows // 2, maps // n_q
    chunks, width = half // TILE, TILE
    devices = n_rows * n_cols
    codes, needed, longest = work_tables(cosines.shape[1] // TILE)
    matrix, each = transform_matrix(npix, devices)
    padded = -(-LEVELS // 128) * 128
    matrix = np.pad(matrix, ((0, 0), (0, padded - LEVELS)))
    basis = (LOW + HIGH - 1, 2 * TILE, TILE)
    vmem = pl.BlockSpec(memory_space=pltpu.VMEM)
    hbm = pl.BlockSpec(memory_space=pltpu.HBM)
    dma = pltpu.SemaphoreType.DMA
    ft, spectra = pl.pallas_call(
        functools.partial(spectra_kernel, n_rows, n_q, codes, needed, longest),
        out_shape=[
            jax.ShapeDtypeStruct((n_q, group, rows), jnp.bfloat16),
            jax.ShapeDtypeStruct((L, maps), jnp.float32),
        ],
        in_specs=[hbm, hbm, hbm, hbm],
        out_specs=[vmem, vmem],
        scratch_shapes=[
            pltpu.VMEM((maps, depth), jnp.bfloat16),
            pltpu.VMEM(matrix.shape, jnp.float32),
            pltpu.VMEM((rows, depth), jnp.bfloat16),
            pltpu.VMEM((chunks, maps, width), jnp.bfloat16),
            pltpu.VMEM((chunks, maps, width), jnp.bfloat16),
            pltpu.VMEM((chunks, n_q, group, width), jnp.float32),
            pltpu.VMEM((chunks, n_q, group, width), jnp.bfloat16),
            pltpu.VMEM((chunks, n_q - 1, group, width), jnp.bfloat16),
            pltpu.VMEM((2 * chunks, n_q, group, width), jnp.bfloat16),
            pltpu.VMEM((chunks, n_q, group, width), jnp.bfloat16),
            pltpu.VMEM((longest + 1, 2 * TILE, TILE), jnp.float32),
            pltpu.VMEM(basis, jnp.bfloat16),
            pltpu.VMEM(basis, jnp.bfloat16),
            pltpu.VMEM((maps, 2 * TILE), jnp.bfloat16),
            pltpu.VMEM((maps, TILE), jnp.float32),
            pltpu.VMEM((LEVELS, maps, TILE // 2), jnp.float32),
            pltpu.VMEM((padded, maps), jnp.float32),
            pltpu.VMEM((devices, each, maps), jnp.float32),
            pltpu.VMEM((devices - 1, each, maps), jnp.float32),
            pltpu.VMEM((each, maps), jnp.float32),
            pltpu.VMEM((devices, each, maps), jnp.float32),
            dma((2,)), dma((2 * chunks,)),
            dma((chunks,)), dma((chunks,)),
            dma((chunks, n_q - 1)), dma((chunks, n_q - 1)),
            dma((chunks, n_q - 1)), dma((chunks, n_q - 1)),
            dma((chunks, n_q)), dma((chunks, n_q)),
            dma((chunks, n_q, n_rows - 1)), dma((chunks, n_q)),
            dma((longest, 2)),
            dma((devices - 1,)), dma((devices - 1,)),
            dma((devices - 1,)), dma((devices - 1,)),
            pltpu.SemaphoreType.REGULAR, pltpu.SemaphoreType.REGULAR,
        ],
        compiler_params=pltpu.CompilerParams(
            collective_id=1, has_side_effects=True, vmem_limit_bytes=52 * 2**20
        ),
        name="spectra",
    )(sky_maps.T, inverse_cov, cosines, jnp.asarray(matrix))
    return (ft.reshape(maps, rows).T, spectra)


def solution(mesh):
    in_specs = (P("prow", "pcol"), P("prow", "pcol"), P("pcol", None))
    out_specs = (P("prow", None), P())
    n_rows, n_cols = mesh.shape["prow"], mesh.shape["pcol"]

    def whole(inverse_cov, cosines, sky_maps):
        npix = cosines.shape[0]
        step = jax.shard_map(
            functools.partial(per_device, npix, n_rows, n_cols),
            mesh=mesh, in_specs=in_specs, out_specs=out_specs, check_vma=False,
        )
        return step(inverse_cov, cosines, sky_maps)

    return whole
```

```python
import functools
import math

import jax
import jax.numpy as jnp
import numpy as np
from jax import lax
from jax.experimental import pallas as pl
from jax.experimental.pallas import tpu as pltpu
from jax.sharding import PartitionSpec as P

L = 64
LMIN = 2
TILE = 256
STRIP = 16
LOW = 11
HIGH = 6
LEVELS = LOW * HIGH
FIELD = 64
LAG = 2
MESH = pl.DeviceIdType.MESH


def transform_matrix(npix, devices):
    top = LMIN + L - 1
    each = -(-L // devices)
    a = [math.comb(2 * k, k) / 4.0**k for k in range(top + 1)]
    product = np.zeros((LEVELS, LEVELS))
    for k in range(LEVELS):
        high, low = divmod(k, LOW)
        product[k, low * HIGH + high] = 1
        if high and low:
            product[k, low * HIGH + high] = 2
            product[k] -= product[high * LOW - low]
    out = np.zeros((devices * each, LEVELS))
    for l in range(LMIN, top + 1):
        owner, place = divmod(l - LMIN, each)
        row = out[owner * each + place]
        for k in range(l + 1):
            row[abs(l - 2 * k)] += a[k] * a[l - k]
        row *= (2 * l + 1) / npix
    return (out @ product).astype(np.float32), each


def pair_up(tiles, n):
    items = []
    for col in range(n):
        mine = sorted((t for t in tiles if t[1] == col), key=lambda t: t[0])
        for k in range(0, len(mine), 2):
            first = mine[k]
            second = mine[k + 1] if k + 1 < len(mine) else (first[0], col, 0)
            items.append((first[0], second[0], first[2], second[2], col))
    return items


def work_tables(n):
    lower = [
        sorted(
            pair_up([(h * n + i, j, 2) for i in range(n) for j in range(n)], n),
            key=lambda t: (t[0], t[4]),
        )
        for h in range(2)
    ]
    own = [(j, j, 1) for j in range(n)] + [(i, 0, 2) for i in range(1, n)]
    if n % 2:
        own += [(i, j, 2) for j in range(1, n) for i in range(j + 1, n)]
    else:
        own += [
            (1 + (j - 1 + d) % (n - 1), j, 2)
            for j in range(1, n) for d in range(1, n // 2)
        ]
    kinds, needed = [], []
    for h in range(2):
        kinds.append(lower[h])
        needed.append(-1)
    for h in range(2):
        kinds.append(lower[1 - h])
        needed.append(0)
    for h in range(2):
        near = sorted(
            pair_up([(h * n + i, j, w) for i, j, w in own], n),
            key=lambda t: max(t[0] - h * n, t[1] - h * n, t[4]),
        )
        far = [
            ((1 - h) * n + i, j, 2)
            for i in range(n) for j in range(n) if (i + j) % 2 == h
        ]
        kinds.append(near + pair_up(far, n))
        needed.append(len(near))
    longest = max(len(k) for k in kinds)
    codes = [
        [row0 + FIELD * (row1 + FIELD * (w0 + FIELD * (w1 + FIELD * col))) for row0, row1, w0, w1, col in k]
        for k in kinds
    ]
    return codes, needed, longest


def spectra_kernel(
    n_rows, n_q, codes, needed, longest, sky, cov_hbm, cos_hbm, matrix_hbm, weighed, out,
    matrix, cov, x_out, x_in, mine, z_out, z_in, ft, fct, xbuf, buf_a, buf_b, lhs, fj, acc,
    sums, parts, landing, summed, shared,
    in_sem, cov_sem, x_send, x_recv, z_send, z_recv, a_send, a_recv, p_send, p_recv, c_send, c_recv,
    tile_sem, s_send, s_recv, g_send, g_recv, row_ready, all_ready,
):
    r = lax.axis_index("prow")
    c = lax.axis_index("pcol")
    q, h = c // 2, c % 2
    maps = sky.shape[0]
    devices = parts.shape[0]
    each = parts.shape[1]
    me = r * (2 * n_q) + c
    group = maps // n_q
    half = cov.shape[0] // 2
    chunks, width = x_out.shape[0], x_out.shape[2]
    partner = (r, c + 1 - 2 * h)
    diagonal = r == q

    def line(k):
        return lax.rem(q + k, n_q)

    def other(k):
        return lax.rem(r + k, n_rows)

    def placed(j):
        return h * chunks + j

    def cov_copy(j, own):
        side = h if own else 1 - h
        return pltpu.make_async_copy(
            cov_hbm.at[pl.ds(pl.multiple_of(side * half + j * width, width), width)],
            cov.at[pl.ds((int(own) * chunks + j) * width, width)],
            cov_sem.at[int(own) * chunks + j],
        )

    def copy(src, dst, send, recv, device):
        return pltpu.make_async_remote_copy(
            src_ref=src, dst_ref=dst, send_sem=send, recv_sem=recv,
            device_id=device, device_id_type=MESH,
        )

    def x_copy(j):
        return copy(x_out.at[j], x_in.at[j], x_send.at[j], x_recv.at[j], partner)

    def z_copy(j, k):
        return copy(
            z_out.at[j, line(k)], z_in.at[j, k - 1],
            z_send.at[j, k - 1], z_recv.at[j, k - 1], (r, line(k) * 2 + h),
        )

    def a_copy(j, k):
        return copy(
            ft.at[placed(j), q], ft.at[placed(j), q],
            a_send.at[j, k - 1], a_recv.at[j, k - 1], (r, line(k) * 2 + h),
        )

    def a_arrival(j, k):
        g = line(n_q - k)
        return g, copy(
            ft.at[placed(j), g], ft.at[placed(j), g],
            a_send.at[j, k - 1], a_recv.at[j, k - 1], partner,
        )

    def p_copy(j, g, slot):
        return copy(
            ft.at[placed(j), g], ft.at[placed(j), g],
            p_send.at[j, slot], p_recv.at[j, slot], partner,
        )

    def c_copy(j, g, slot, k):
        return copy(
            ft.at[placed(j), g], fct.at[j, g],
            c_send.at[j, slot, k - 1], c_recv.at[j, slot], (other(k), c),
        )

    def product(j, own):
        cov_copy(j, own).wait()
        block = cov[(int(own) * chunks + j) * width : (int(own) * chunks + j + 1) * width, :]
        return lax.dot_general(
            sky[...], block, (((1,), (1,)), ((), ())), preferred_element_type=jnp.float32
        )

    def share(j, g, slot):
        @pl.when(diagonal)
        def _():
            for k in range(1, n_rows):
                c_copy(j, g, slot, k).start()

        p_copy(j, g, slot).start()

    def pass_on(j):
        for k in range(1, n_q):
            g, arrival = a_arrival(j, k)
            arrival.wait_recv()
            share(j, g, k)

        @pl.when(diagonal)
        def _():
            fct[j] = ft[placed(j)]

    kind = jnp.where(r > q, h, jnp.where(r < q, 2 + h, 4 + h))
    n_strips = 2 * TILE // STRIP

    def by_kind(values):
        chosen = jnp.int32(values[0])
        for i in range(1, len(values)):
            chosen = jnp.where(kind == i, jnp.int32(values[i]), chosen)
        return chosen

    n_items = by_kind([len(k) for k in codes])
    other_from = by_kind(needed)
    item_codes = [by_kind([k[i] if i < len(k) else k[0] for k in codes]) for i in range(longest)]

    def fields(item):
        code = item_codes[0]
        for i in range(1, longest):
            code = jnp.where(item == i, item_codes[i], code)
        found = []
        for _ in range(5):
            found.append(code % FIELD)
            code = code // FIELD
        return found

    def tile_copies(item):
        row0, row1, _, _, col = fields(item)
        for side, row in enumerate((row0, row1)):
            yield pltpu.make_async_copy(
                cos_hbm.at[
                    pl.ds(pl.multiple_of(row * TILE, TILE), TILE),
                    pl.ds(pl.multiple_of(col * TILE, TILE), TILE),
                ],
                xbuf.at[item, pl.ds(side * TILE, TILE)],
                tile_sem.at[item, side],
            )

    def fetch(item, carry):
        for tile in tile_copies(item):
            tile.start()
        return carry

    def landed(item):
        @pl.when(item < n_items)
        def _():
            for tile in tile_copies(item):
                tile.wait()

    def set_operands(item):
        row0, row1, w0, w1, col = fields(item)
        for side, (row, weight) in enumerate(((row0, w0), (row1, w1))):
            value = [ft[row, g].astype(jnp.float32) for g in range(n_q)]
            value = jnp.concatenate(value, axis=0) * weight.astype(jnp.float32)
            lhs[:, side * TILE : (side + 1) * TILE] = value.astype(jnp.bfloat16)
        for g in range(n_q):
            fj[g * group : (g + 1) * group] = fct[col, g].astype(jnp.float32)

    def gen_strip(buf, item, s):
        rows = pl.ds(pl.multiple_of(s * STRIP, STRIP), STRIP)
        x = xbuf[item, rows, :]
        xx = x + x
        buf[1, rows, :] = x.astype(jnp.bfloat16)
        p, t = x, xx * x - 1.0
        for k in range(2, LOW):
            buf[k, rows, :] = t.astype(jnp.bfloat16)
            p, t = t, xx * t - p
        yy = t + t
        buf[LOW, rows, :] = t.astype(jnp.bfloat16)
        p, t = t, yy * t - 1.0
        for k in range(2, HIGH):
            buf[LOW + k - 1, rows, :] = t.astype(jnp.bfloat16)
            p, t = t, yy * t - p

    def item_pass(item, use, gen):
        following = jnp.minimum(item + 1, n_items - 1)
        landed(item + 1)

        for j in range(max(LAG, chunks - LAG), chunks):
            @pl.when(item == j - 1)
            def _():
                pass_on(j)

        @pl.when(jnp.logical_and(jnp.logical_not(diagonal), item < chunks))
        def _():
            for slot in range(n_q):
                copy(
                    ft.at[placed(0), q], fct.at[item, mirrored(slot)],
                    c_send.at[0, slot, 0], c_recv.at[item, slot], partner,
                ).wait_recv()

        @pl.when(jnp.logical_and(r < q, item % chunks == 0))
        def _():
            for i in range(2):
                for slot in range(n_q):
                    elsewhere(item // chunks * 2 + i, slot).wait_recv()

        @pl.when(jnp.logical_and(diagonal, item == other_from))
        def _():
            other_half()

        set_operands(item)

        half_tile = TILE // 2
        done = 0
        for level in range(LEVELS):
            k, g = divmod(level, HIGH)
            upto = (level + 1) * n_strips // LEVELS
            for s in range(done, upto):
                gen_strip(gen, following, s)
            done = upto
            if k == 0:
                rhs = use[LOW + g - 1] if g else use[0]
            else:
                rhs = use[LOW + g - 1] * use[k] if g else use[k]
            image = jnp.dot(lhs[...], rhs, preferred_element_type=jnp.float32)
            prod = image * fj[...]
            folded = prod[:, :half_tile] + prod[:, half_tile:]
            acc[level] += folded
            if (level + 2) * n_strips // LEVELS > upto:
                xbuf[longest, 0:8, 0:half_tile] = folded[0:8, :]

    def first_strip(s, carry):
        gen_strip(buf_a, 0, s)
        return carry

    def two_items(pair, carry):
        item_pass(2 * pair, buf_a, buf_b)

        @pl.when(2 * pair + 1 < n_items)
        def _():
            item_pass(2 * pair + 1, buf_b, buf_a)

        return carry

    def member(k):
        device = lax.rem(me + k, devices)
        return (device // (2 * n_q), device % (2 * n_q))

    def each_other(body):
        lax.fori_loop(1, devices, lambda k, carry: (body(k), carry)[1], 0)

    def scatter(k):
        return copy(
            parts.at[lax.rem(me + k, devices)], landing.at[k - 1],
            s_send.at[k - 1], s_recv.at[k - 1], member(k),
        )

    def gather(k, slot):
        return copy(
            summed, shared.at[slot], g_send.at[k - 1], g_recv.at[k - 1], member(k)
        )

    def elsewhere(j, slot):
        g = mirrored(slot)
        where = (1 - h) * chunks + j
        return copy(
            ft.at[where, g], ft.at[where, g],
            p_send.at[j, slot], p_recv.at[j, slot], partner,
        )

    def other_half():
        for j in range(chunks):
            for slot in range(n_q):
                elsewhere(j, slot).wait_recv()

    def mirrored(slot):
        return q if slot == 0 else line(n_q - slot)

    matrix_copy = pltpu.make_async_copy(
        matrix_hbm.at[pl.ds(0, matrix.shape[0])], matrix, in_sem
    )
    for own in (False, True):
        for j in range(chunks):
            cov_copy(j, own).start()
    matrix_copy.start()
    lax.fori_loop(0, n_items, fetch, 0)
    barrier = pltpu.get_barrier_semaphore()
    greeted = [partner]
    greeted += [(r, line(k) * 2 + h) for k in range(1, n_q)]
    greeted += [(other(k), c) for k in range(1, n_rows)]
    for device in greeted:
        pl.semaphore_signal(barrier, inc=1, device_id=device, device_id_type=MESH)
    for j in range(chunks):
        x_out[j] = product(j, False).astype(x_out.dtype)
        if j == 0:
            pl.semaphore_wait(barrier, len(greeted))
            pl.semaphore_signal(row_ready, inc=1, device_id=partner, device_id_type=MESH)
        x_copy(j).start()
    for j in range(chunks):
        total = product(j, True)
        for g in range(n_q):
            mine[j, g] = total[g * group : (g + 1) * group]
    acc[...] = jnp.zeros_like(acc)
    for buf in (buf_a, buf_b):
        buf[0] = jnp.ones(buf.shape[1:], buf.dtype)
    landed(0)
    lax.fori_loop(0, n_strips, first_strip, 0, unroll=4)
    pl.semaphore_wait(row_ready, 1)
    for k in range(1, n_rows):
        pl.semaphore_signal(all_ready, inc=1, device_id=(other(k), c), device_id_type=MESH)
    for j in range(chunks):
        x_copy(j).wait_recv()
        for g in range(n_q):
            total = mine[j, g] + x_in[j, g * group : (g + 1) * group]
            mine[j, g] = total
            z_out[j, g] = total.astype(z_out.dtype)
        for k in range(1, n_q):
            z_copy(j, k).start()
    for j in range(chunks):
        total = mine[j, q]
        for k in range(1, n_q):
            z_copy(j, k).wait_recv()
            total = total + z_in[j, k - 1]
        ft[placed(j), q] = total.astype(ft.dtype)
        for k in range(1, n_q):
            a_copy(j, k).start()
        share(j, q, 0)
        if j >= LAG:
            pass_on(j - LAG)
    for j in range(max(chunks - LAG, 0), min(LAG, chunks)):
        pass_on(j)
    lax.fori_loop(0, (n_items + 1) // 2, two_items, 0)
    sums[...] = jnp.zeros_like(sums)
    sums[0:LEVELS, :] = jnp.sum(acc[...], axis=-1)
    matrix_copy.wait()
    spectra = jnp.dot(
        matrix[...], sums[...],
        precision=lax.Precision.HIGHEST, preferred_element_type=jnp.float32,
    )
    for i in range(devices):
        parts[i] = spectra[i * each : (i + 1) * each]
    pl.semaphore_wait(all_ready, n_rows - 1)
    each_other(lambda k: scatter(k).start())

    @pl.when(r > q)
    def _():
        other_half()

    for t in range(2 * chunks):
        for g in range(n_q):
            weighed[g, :, t * width : (t + 1) * width] = ft[t, g]
    @pl.when(diagonal)
    def _():
        for j in range(chunks):
            for slot in range(n_q):
                for k in range(1, n_rows):
                    c_copy(j, mirrored(slot), slot, k).wait_send()

    for j in range(chunks):
        x_copy(j).wait_send()
        for k in range(1, n_q):
            z_copy(j, k).wait_send()
            a_copy(j, k).wait_send()
        for slot in range(n_q):
            p_copy(j, mirrored(slot), slot).wait_send()
    each_other(lambda k: scatter(k).wait_recv())
    summed[...] = lax.fori_loop(0, devices - 1, lambda k, t: t + landing[k], parts[me])
    each_other(lambda k: gather(k, me).start())
    shared[me] = summed[...]
    each_other(lambda k: gather(k, lax.rem(me - k + devices, devices)).wait_recv())
    for i in range(devices):
        if i * each < out.shape[0]:
            out[i * each : (i + 1) * each, :] = shared[i]
    each_other(lambda k: scatter(k).wait_send())
    each_other(lambda k: gather(k, me).wait_send())


def per_device(npix, n_rows, n_cols, inverse_cov, cosines, sky_maps):
    depth, maps = sky_maps.shape
    rows = inverse_cov.shape[0]
    n_q = n_cols // 2
    half, group = rows // 2, maps // n_q
    chunks, width = half // TILE, TILE
    devices = n_rows * n_cols
    codes, needed, longest = work_tables(cosines.shape[1] // TILE)
    matrix, each = transform_matrix(npix, devices)
    padded = -(-LEVELS // 128) * 128
    matrix = np.pad(matrix, ((0, 4096 - matrix.shape[0]), (0, padded - LEVELS)))
    basis = (LOW + HIGH - 1, 2 * TILE, TILE)
    vmem = pl.BlockSpec(memory_space=pltpu.VMEM)
    hbm = pl.BlockSpec(memory_space=pl.ANY)
    dma = pltpu.SemaphoreType.DMA
    ft, spectra = pl.pallas_call(
        functools.partial(spectra_kernel, n_rows, n_q, codes, needed, longest),
        out_shape=[
            jax.ShapeDtypeStruct((n_q, group, rows), jnp.bfloat16),
            jax.ShapeDtypeStruct((L, maps), jnp.float32),
        ],
        in_specs=[vmem, hbm, hbm, hbm],
        out_specs=[vmem, vmem],
        scratch_shapes=[
            pltpu.VMEM((devices * each, padded), jnp.float32),
            pltpu.VMEM((rows, depth), jnp.bfloat16),
            pltpu.VMEM((chunks, maps, width), jnp.bfloat16),
            pltpu.VMEM((chunks, maps, width), jnp.bfloat16),
            pltpu.VMEM((chunks, n_q, group, width), jnp.float32),
            pltpu.VMEM((chunks, n_q, group, width), jnp.bfloat16),
            pltpu.VMEM((chunks, n_q - 1, group, width), jnp.bfloat16),
            pltpu.VMEM((2 * chunks, n_q, group, width), jnp.bfloat16),
            pltpu.VMEM((chunks, n_q, group, width), jnp.bfloat16),
            pltpu.VMEM((longest + 1, 2 * TILE, TILE), jnp.float32),
            pltpu.VMEM(basis, jnp.bfloat16),
            pltpu.VMEM(basis, jnp.bfloat16),
            pltpu.VMEM((maps, 2 * TILE), jnp.bfloat16),
            pltpu.VMEM((maps, TILE), jnp.float32),
            pltpu.VMEM((LEVELS, maps, TILE // 2), jnp.float32),
            pltpu.VMEM((padded, maps), jnp.float32),
            pltpu.VMEM((devices, each, maps), jnp.float32),
            pltpu.VMEM((devices - 1, each, maps), jnp.float32),
            pltpu.VMEM((each, maps), jnp.float32),
            pltpu.VMEM((devices, each, maps), jnp.float32),
            dma, dma((2 * chunks,)),
            dma((chunks,)), dma((chunks,)),
            dma((chunks, n_q - 1)), dma((chunks, n_q - 1)),
            dma((chunks, n_q - 1)), dma((chunks, n_q - 1)),
            dma((chunks, n_q)), dma((chunks, n_q)),
            dma((chunks, n_q, n_rows - 1)), dma((chunks, n_q)),
            dma((longest, 2)),
            dma((devices - 1,)), dma((devices - 1,)),
            dma((devices - 1,)), dma((devices - 1,)),
            pltpu.SemaphoreType.REGULAR, pltpu.SemaphoreType.REGULAR,
        ],
        compiler_params=pltpu.CompilerParams(
            collective_id=1, has_side_effects=True, vmem_limit_bytes=52 * 2**20
        ),
        name="spectra",
    )(sky_maps.T, inverse_cov, cosines, jnp.asarray(matrix))
    return (ft.reshape(maps, rows).T, spectra)


def solution(mesh):
    in_specs = (P("prow", "pcol"), P("prow", "pcol"), P("pcol", None))
    out_specs = (P("prow", None), P())
    n_rows, n_cols = mesh.shape["prow"], mesh.shape["pcol"]

    def whole(inverse_cov, cosines, sky_maps):
        npix = cosines.shape[0]
        step = jax.shard_map(
            functools.partial(per_device, npix, n_rows, n_cols),
            mesh=mesh, in_specs=in_specs, out_specs=out_specs, check_vma=False,
        )
        return step(inverse_cov, cosines, sky_maps)

    return whole
```

```python
import functools
import math

import jax
import jax.numpy as jnp
import numpy as np
from jax import lax
from jax.experimental import pallas as pl
from jax.experimental.pallas import tpu as pltpu
from jax.sharding import PartitionSpec as P

L = 64
LMIN = 2
TILE = 256
STRIP = 16
LOW = 11
HIGH = 6
LEVELS = LOW * HIGH
FIELD = 64
LAG = 2
MESH = pl.DeviceIdType.MESH


def transform_matrix(npix, devices):
    top = LMIN + L - 1
    each = -(-L // devices)
    a = [math.comb(2 * k, k) / 4.0**k for k in range(top + 1)]
    product = np.zeros((LEVELS, LEVELS))
    for k in range(LEVELS):
        high, low = divmod(k, LOW)
        product[k, low * HIGH + high] = 1
        if high and low:
            product[k, low * HIGH + high] = 2
            product[k] -= product[high * LOW - low]
    out = np.zeros((devices * each, LEVELS))
    for l in range(LMIN, top + 1):
        owner, place = divmod(l - LMIN, each)
        row = out[owner * each + place]
        for k in range(l + 1):
            row[abs(l - 2 * k)] += a[k] * a[l - k]
        row *= (2 * l + 1) / npix
    return (out @ product).astype(np.float32), each


def pair_up(tiles, n):
    items = []
    for col in range(n):
        mine = sorted((t for t in tiles if t[1] == col), key=lambda t: t[0])
        for k in range(0, len(mine), 2):
            first = mine[k]
            second = mine[k + 1] if k + 1 < len(mine) else (first[0], col, 0)
            items.append((first[0], second[0], first[2], second[2], col))
    return items


def work_tables(n):
    lower = [
        sorted(
            pair_up([(h * n + i, j, 2) for i in range(n) for j in range(n)], n),
            key=lambda t: (t[0], t[4]),
        )
        for h in range(2)
    ]
    own = [(j, j, 1) for j in range(n)] + [(i, 0, 2) for i in range(1, n)]
    if n % 2:
        own += [(i, j, 2) for j in range(1, n) for i in range(j + 1, n)]
    else:
        own += [
            (1 + (j - 1 + d) % (n - 1), j, 2)
            for j in range(1, n) for d in range(1, n // 2)
        ]
    kinds, needed = [], []
    for h in range(2):
        kinds.append(lower[h])
        needed.append(-1)
    for h in range(2):
        kinds.append(lower[1 - h])
        needed.append(0)
    for h in range(2):
        near = sorted(
            pair_up([(h * n + i, j, w) for i, j, w in own], n),
            key=lambda t: max(t[0] - h * n, t[1] - h * n, t[4]),
        )
        far = [
            ((1 - h) * n + i, j, 2)
            for i in range(n) for j in range(n) if (i + j) % 2 == h
        ]
        kinds.append(near + pair_up(far, n))
        needed.append(len(near))
    longest = max(len(k) for k in kinds)
    codes = [
        [row0 + FIELD * (row1 + FIELD * (w0 + FIELD * (w1 + FIELD * col))) for row0, row1, w0, w1, col in k]
        for k in kinds
    ]
    return codes, needed, longest


def spectra_kernel(
    n_rows, n_q, codes, needed, longest, sky, cov_hbm, cos_hbm, matrix_hbm, weighed, out,
    matrix, cov, x_out, x_in, mine, z_out, z_in, ft, fct, xbuf, buf_a, buf_b, lhs, fj, acc,
    sums, parts, landing, summed, shared,
    in_sem, cov_sem, x_send, x_recv, z_send, z_recv, a_send, a_recv, p_send, p_recv, c_send, c_recv,
    tile_sem, s_send, s_recv, g_send, g_recv, row_ready, all_ready,
):
    r = lax.axis_index("prow")
    c = lax.axis_index("pcol")
    q, h = c // 2, c % 2
    maps = sky.shape[0]
    devices = parts.shape[0]
    each = parts.shape[1]
    me = r * (2 * n_q) + c
    group = maps // n_q
    half = cov.shape[0] // 2
    chunks, width = x_out.shape[0], x_out.shape[2]
    partner = (r, c + 1 - 2 * h)
    diagonal = r == q

    def line(k):
        return lax.rem(q + k, n_q)

    def other(k):
        return lax.rem(r + k, n_rows)

    def placed(j):
        return h * chunks + j

    def cov_copy(j, own):
        side = h if own else 1 - h
        return pltpu.make_async_copy(
            cov_hbm.at[pl.ds(pl.multiple_of(side * half + j * width, width), width)],
            cov.at[pl.ds((int(own) * chunks + j) * width, width)],
            cov_sem.at[int(own) * chunks + j],
        )

    def copy(src, dst, send, recv, device):
        return pltpu.make_async_remote_copy(
            src_ref=src, dst_ref=dst, send_sem=send, recv_sem=recv,
            device_id=device, device_id_type=MESH,
        )

    def x_copy(j):
        return copy(x_out.at[j], x_in.at[j], x_send.at[j], x_recv.at[j], partner)

    def z_copy(j, k):
        return copy(
            z_out.at[j, line(k)], z_in.at[j, k - 1],
            z_send.at[j, k - 1], z_recv.at[j, k - 1], (r, line(k) * 2 + h),
        )

    def a_copy(j, k):
        return copy(
            ft.at[placed(j), q], ft.at[placed(j), q],
            a_send.at[j, k - 1], a_recv.at[j, k - 1], (r, line(k) * 2 + h),
        )

    def a_arrival(j, k):
        g = line(n_q - k)
        return g, copy(
            ft.at[placed(j), g], ft.at[placed(j), g],
            a_send.at[j, k - 1], a_recv.at[j, k - 1], partner,
        )

    def p_copy(j, g, slot):
        return copy(
            ft.at[placed(j), g], ft.at[placed(j), g],
            p_send.at[j, slot], p_recv.at[j, slot], partner,
        )

    def c_copy(j, g, slot, k):
        return copy(
            ft.at[placed(j), g], fct.at[j, g],
            c_send.at[j, slot, k - 1], c_recv.at[j, slot], (other(k), c),
        )

    def product(j, own):
        cov_copy(j, own).wait()
        block = cov[(int(own) * chunks + j) * width : (int(own) * chunks + j + 1) * width, :]
        return lax.dot_general(
            sky[...], block, (((1,), (1,)), ((), ())), preferred_element_type=jnp.float32
        )

    def share(j, g, slot):
        @pl.when(diagonal)
        def _():
            for k in range(1, n_rows):
                c_copy(j, g, slot, k).start()

        p_copy(j, g, slot).start()

    def pass_on(j):
        for k in range(1, n_q):
            g, arrival = a_arrival(j, k)
            arrival.wait_recv()
            share(j, g, k)

        @pl.when(diagonal)
        def _():
            fct[j] = ft[placed(j)]

    kind = jnp.where(r > q, h, jnp.where(r < q, 2 + h, 4 + h))
    n_strips = 2 * TILE // STRIP

    def by_kind(values):
        chosen = jnp.int32(values[0])
        for i in range(1, len(values)):
            chosen = jnp.where(kind == i, jnp.int32(values[i]), chosen)
        return chosen

    n_items = by_kind([len(k) for k in codes])
    other_from = by_kind(needed)
    item_codes = [by_kind([k[i] if i < len(k) else k[0] for k in codes]) for i in range(longest)]

    def fields(item):
        code = item_codes[0]
        for i in range(1, longest):
            code = jnp.where(item == i, item_codes[i], code)
        found = []
        for _ in range(5):
            found.append(code % FIELD)
            code = code // FIELD
        return found

    def tile_copies(item):
        row0, row1, _, _, col = fields(item)
        for side, row in enumerate((row0, row1)):
            yield pltpu.make_async_copy(
                cos_hbm.at[
                    pl.ds(pl.multiple_of(row * TILE, TILE), TILE),
                    pl.ds(pl.multiple_of(col * TILE, TILE), TILE),
                ],
                xbuf.at[item, pl.ds(side * TILE, TILE)],
                tile_sem.at[item, side],
            )

    def fetch(item, carry):
        for tile in tile_copies(item):
            tile.start()
        return carry

    def landed(item):
        @pl.when(item < n_items)
        def _():
            for tile in tile_copies(item):
                tile.wait()

    def set_operands(item):
        row0, row1, w0, w1, col = fields(item)
        for side, (row, weight) in enumerate(((row0, w0), (row1, w1))):
            value = [ft[row, g].astype(jnp.float32) for g in range(n_q)]
            value = jnp.concatenate(value, axis=0) * weight.astype(jnp.float32)
            lhs[:, side * TILE : (side + 1) * TILE] = value.astype(jnp.bfloat16)
        for g in range(n_q):
            fj[g * group : (g + 1) * group] = fct[col, g].astype(jnp.float32)

    def gen_strip(buf, item, s):
        rows = pl.ds(pl.multiple_of(s * STRIP, STRIP), STRIP)
        x = xbuf[item, rows, :]
        xx = x + x
        buf[1, rows, :] = x.astype(jnp.bfloat16)
        p, t = x, xx * x - 1.0
        for k in range(2, LOW):
            buf[k, rows, :] = t.astype(jnp.bfloat16)
            p, t = t, xx * t - p
        yy = t + t
        buf[LOW, rows, :] = t.astype(jnp.bfloat16)
        p, t = t, yy * t - 1.0
        for k in range(2, HIGH):
            buf[LOW + k - 1, rows, :] = t.astype(jnp.bfloat16)
            p, t = t, yy * t - p

    def item_pass(item, use, gen):
        following = jnp.minimum(item + 1, n_items - 1)
        landed(item + 1)

        for j in range(max(LAG, chunks - LAG), chunks):
            @pl.when(item == j - 1)
            def _():
                pass_on(j)

        @pl.when(jnp.logical_and(jnp.logical_not(diagonal), item < chunks))
        def _():
            for slot in range(n_q):
                copy(
                    ft.at[placed(0), q], fct.at[item, mirrored(slot)],
                    c_send.at[0, slot, 0], c_recv.at[item, slot], partner,
                ).wait_recv()

        @pl.when(jnp.logical_and(r < q, item % chunks == 0))
        def _():
            for i in range(2):
                for slot in range(n_q):
                    elsewhere(item // chunks * 2 + i, slot).wait_recv()

        @pl.when(jnp.logical_and(diagonal, item == other_from))
        def _():
            other_half()

        set_operands(item)

        half_tile = TILE // 2
        done = 0
        for level in range(LEVELS):
            k, g = divmod(level, HIGH)
            upto = (level + 1) * n_strips // LEVELS
            for s in range(done, upto):
                gen_strip(gen, following, s)
            done = upto
            if k == 0:
                rhs = use[LOW + g - 1] if g else use[0]
            else:
                rhs = use[LOW + g - 1] * use[k] if g else use[k]
            image = jnp.dot(lhs[...], rhs, preferred_element_type=jnp.float32)
            prod = image * fj[...]
            folded = prod[:, :half_tile] + prod[:, half_tile:]
            acc[level] += folded
            if (level + 2) * n_strips // LEVELS > upto:
                xbuf[longest, 0:8, 0:half_tile] = folded[0:8, :]

    def first_strip(s, carry):
        gen_strip(buf_a, 0, s)
        return carry

    def two_items(pair, carry):
        item_pass(2 * pair, buf_a, buf_b)

        @pl.when(2 * pair + 1 < n_items)
        def _():
            item_pass(2 * pair + 1, buf_b, buf_a)

        return carry

    def member(k):
        device = lax.rem(me + k, devices)
        return (device // (2 * n_q), device % (2 * n_q))

    def each_other(body):
        if devices > 32:
            lax.fori_loop(1, devices, lambda k, carry: (body(k), carry)[1], 0)
        else:
            for k in range(1, devices):
                body(k)

    def scatter(k):
        return copy(
            parts.at[lax.rem(me + k, devices)], landing.at[k - 1],
            s_send.at[k - 1], s_recv.at[k - 1], member(k),
        )

    def gather(k, slot):
        return copy(
            summed, shared.at[slot], g_send.at[k - 1], g_recv.at[k - 1], member(k)
        )

    def elsewhere(j, slot):
        g = mirrored(slot)
        where = (1 - h) * chunks + j
        return copy(
            ft.at[where, g], ft.at[where, g],
            p_send.at[j, slot], p_recv.at[j, slot], partner,
        )

    def other_half():
        for j in range(chunks):
            for slot in range(n_q):
                elsewhere(j, slot).wait_recv()

    def mirrored(slot):
        return q if slot == 0 else line(n_q - slot)

    matrix_copy = pltpu.make_async_copy(
        matrix_hbm.at[pl.ds(0, matrix.shape[0])], matrix, in_sem
    )
    for own in (False, True):
        for j in range(chunks):
            cov_copy(j, own).start()
    matrix_copy.start()
    lax.fori_loop(0, n_items, fetch, 0)
    barrier = pltpu.get_barrier_semaphore()
    greeted = [partner]
    greeted += [(r, line(k) * 2 + h) for k in range(1, n_q)]
    greeted += [(other(k), c) for k in range(1, n_rows)]
    for device in greeted:
        pl.semaphore_signal(barrier, inc=1, device_id=device, device_id_type=MESH)
    for j in range(chunks):
        x_out[j] = product(j, False).astype(x_out.dtype)
        if j == 0:
            pl.semaphore_wait(barrier, len(greeted))
            pl.semaphore_signal(row_ready, inc=1, device_id=partner, device_id_type=MESH)
        x_copy(j).start()
    for j in range(chunks):
        total = product(j, True)
        for g in range(n_q):
            mine[j, g] = total[g * group : (g + 1) * group]
    acc[...] = jnp.zeros_like(acc)
    for buf in (buf_a, buf_b):
        buf[0] = jnp.ones(buf.shape[1:], buf.dtype)
    landed(0)
    lax.fori_loop(0, n_strips, first_strip, 0, unroll=4)
    pl.semaphore_wait(row_ready, 1)
    for k in range(1, n_rows):
        pl.semaphore_signal(all_ready, inc=1, device_id=(other(k), c), device_id_type=MESH)
    for j in range(chunks):
        x_copy(j).wait_recv()
        for g in range(n_q):
            total = mine[j, g] + x_in[j, g * group : (g + 1) * group]
            mine[j, g] = total
            z_out[j, g] = total.astype(z_out.dtype)
        for k in range(1, n_q):
            z_copy(j, k).start()
    for j in range(chunks):
        total = mine[j, q]
        for k in range(1, n_q):
            z_copy(j, k).wait_recv()
            total = total + z_in[j, k - 1]
        ft[placed(j), q] = total.astype(ft.dtype)
        for k in range(1, n_q):
            a_copy(j, k).start()
        share(j, q, 0)
        if j >= LAG:
            pass_on(j - LAG)
    for j in range(max(chunks - LAG, 0), min(LAG, chunks)):
        pass_on(j)
    lax.fori_loop(0, (n_items + 1) // 2, two_items, 0)
    sums[...] = jnp.zeros_like(sums)
    sums[0:LEVELS, :] = jnp.sum(acc[...], axis=-1)
    matrix_copy.wait()
    spectra = jnp.dot(
        matrix[...], sums[...],
        precision=lax.Precision.HIGHEST, preferred_element_type=jnp.float32,
    )
    for i in range(devices):
        parts[i] = spectra[i * each : (i + 1) * each]
    pl.semaphore_wait(all_ready, n_rows - 1)
    each_other(lambda k: scatter(k).start())

    @pl.when(r > q)
    def _():
        other_half()

    for t in range(2 * chunks):
        for g in range(n_q):
            weighed[g, :, t * width : (t + 1) * width] = ft[t, g]
    @pl.when(diagonal)
    def _():
        for j in range(chunks):
            for slot in range(n_q):
                for k in range(1, n_rows):
                    c_copy(j, mirrored(slot), slot, k).wait_send()

    for j in range(chunks):
        x_copy(j).wait_send()
        for k in range(1, n_q):
            z_copy(j, k).wait_send()
            a_copy(j, k).wait_send()
        for slot in range(n_q):
            p_copy(j, mirrored(slot), slot).wait_send()
    each_other(lambda k: scatter(k).wait_recv())
    summed[...] = lax.fori_loop(0, devices - 1, lambda k, t: t + landing[k], parts[me])
    each_other(lambda k: gather(k, me).start())
    shared[me] = summed[...]
    each_other(lambda k: gather(k, lax.rem(me - k + devices, devices)).wait_recv())
    for i in range(devices):
        if i * each < out.shape[0]:
            out[i * each : (i + 1) * each, :] = shared[i]
    each_other(lambda k: scatter(k).wait_send())
    each_other(lambda k: gather(k, me).wait_send())


def per_device(npix, n_rows, n_cols, inverse_cov, cosines, sky_maps):
    depth, maps = sky_maps.shape
    rows = inverse_cov.shape[0]
    n_q = n_cols // 2
    half, group = rows // 2, maps // n_q
    chunks, width = half // TILE, TILE
    devices = n_rows * n_cols
    codes, needed, longest = work_tables(cosines.shape[1] // TILE)
    matrix, each = transform_matrix(npix, devices)
    padded = -(-LEVELS // 128) * 128
    matrix = np.pad(matrix, ((0, 4096 - matrix.shape[0]), (0, padded - LEVELS)))
    basis = (LOW + HIGH - 1, 2 * TILE, TILE)
    vmem = pl.BlockSpec(memory_space=pltpu.VMEM)
    hbm = pl.BlockSpec(memory_space=pl.ANY)
    dma = pltpu.SemaphoreType.DMA
    ft, spectra = pl.pallas_call(
        functools.partial(spectra_kernel, n_rows, n_q, codes, needed, longest),
        out_shape=[
            jax.ShapeDtypeStruct((n_q, group, rows), jnp.bfloat16),
            jax.ShapeDtypeStruct((L, maps), jnp.float32),
        ],
        in_specs=[vmem, hbm, hbm, hbm],
        out_specs=[vmem, vmem],
        scratch_shapes=[
            pltpu.VMEM((devices * each, padded), jnp.float32),
            pltpu.VMEM((rows, depth), jnp.bfloat16),
            pltpu.VMEM((chunks, maps, width), jnp.bfloat16),
            pltpu.VMEM((chunks, maps, width), jnp.bfloat16),
            pltpu.VMEM((chunks, n_q, group, width), jnp.float32),
            pltpu.VMEM((chunks, n_q, group, width), jnp.bfloat16),
            pltpu.VMEM((chunks, n_q - 1, group, width), jnp.bfloat16),
            pltpu.VMEM((2 * chunks, n_q, group, width), jnp.bfloat16),
            pltpu.VMEM((chunks, n_q, group, width), jnp.bfloat16),
            pltpu.VMEM((longest + 1, 2 * TILE, TILE), jnp.float32),
            pltpu.VMEM(basis, jnp.bfloat16),
            pltpu.VMEM(basis, jnp.bfloat16),
            pltpu.VMEM((maps, 2 * TILE), jnp.bfloat16),
            pltpu.VMEM((maps, TILE), jnp.float32),
            pltpu.VMEM((LEVELS, maps, TILE // 2), jnp.float32),
            pltpu.VMEM((padded, maps), jnp.float32),
            pltpu.VMEM((devices, each, maps), jnp.float32),
            pltpu.VMEM((devices - 1, each, maps), jnp.float32),
            pltpu.VMEM((each, maps), jnp.float32),
            pltpu.VMEM((devices, each, maps), jnp.float32),
            dma, dma((2 * chunks,)),
            dma((chunks,)), dma((chunks,)),
            dma((chunks, n_q - 1)), dma((chunks, n_q - 1)),
            dma((chunks, n_q - 1)), dma((chunks, n_q - 1)),
            dma((chunks, n_q)), dma((chunks, n_q)),
            dma((chunks, n_q, n_rows - 1)), dma((chunks, n_q)),
            dma((longest, 2)),
            dma((devices - 1,)), dma((devices - 1,)),
            dma((devices - 1,)), dma((devices - 1,)),
            pltpu.SemaphoreType.REGULAR, pltpu.SemaphoreType.REGULAR,
        ],
        compiler_params=pltpu.CompilerParams(
            collective_id=1, has_side_effects=True, vmem_limit_bytes=52 * 2**20
        ),
        name="spectra",
    )(sky_maps.T, inverse_cov, cosines, jnp.asarray(matrix))
    return (ft.reshape(maps, rows).T, spectra)


def solution(mesh):
    in_specs = (P("prow", "pcol"), P("prow", "pcol"), P("pcol", None))
    out_specs = (P("prow", None), P())
    n_rows, n_cols = mesh.shape["prow"], mesh.shape["pcol"]

    def whole(inverse_cov, cosines, sky_maps):
        npix = cosines.shape[0]
        step = jax.shard_map(
            functools.partial(per_device, npix, n_rows, n_cols),
            mesh=mesh, in_specs=in_specs, out_specs=out_specs, check_vma=False,
        )
        return step(inverse_cov, cosines, sky_maps)

    return whole
```
